8 devices in a mesh: dp: 1 (over z), ep: 8 (over y, x, core).
Axes of the slice: x: 2, y: 2, z: 1, core: 2. Of those that a mesh axis runs over, the one named last changes fastest.
Arguments:
- tokens: bfloat16 [24576, 1024], P(('dp', 'ep'))
- expert_idx: int32 [24576], P(('dp', 'ep'))
- w_router: float32 [1024, 128], replicated
- w_in: bfloat16 [128, 1024, 2816], P('ep')
- w_out: bfloat16 [128, 2816, 1024], P('ep')
Outputs:
- output: bfloat16 [24576, 1024], P(('dp', 'ep'))
All inputs are finite; a program needn't handle non-finite values.
Results may differ from the reference program's by a relative error of at most 0.00104.
Values are sent between devices in bfloat16 or wider.
A program may use at most 1 GiB of HBM per device.

```python
import jax
import jax.numpy as jnp
from jax import lax

MODEL_DIM = 1024
HIDDEN_DIM = 2816
NUM_EXPERTS = 128
GROUP_TOKENS = 3072
NUM_GROUPS = 8
CAPACITY = (5 * GROUP_TOKENS + 4 * NUM_EXPERTS - 1) // (4 * NUM_EXPERTS)
TOTAL_TOKENS = NUM_GROUPS * GROUP_TOKENS


def draw_choices(key):
    key_perm, key_shift, key_redraw, key_pick, key_hot = jax.random.split(key, 5)
    balanced = jnp.arange(GROUP_TOKENS, dtype=jnp.int32) % NUM_EXPERTS
    perm_keys = jax.random.split(key_perm, NUM_GROUPS)
    shuffled = jax.vmap(lambda perm_key: jax.random.permutation(perm_key, balanced))(perm_keys)
    group_shift = jax.random.randint(key_shift, (NUM_GROUPS, 1), 0, NUM_EXPERTS)
    choice = (shuffled + group_shift) % NUM_EXPERTS
    redraw = jax.random.randint(key_redraw, (NUM_GROUPS, GROUP_TOKENS), 0, 8) == 0
    picked = jax.random.randint(key_pick, (NUM_GROUPS, GROUP_TOKENS), 0, NUM_EXPERTS)
    choice = jnp.where(redraw, picked, choice)
    hot_expert = jax.random.randint(key_hot, (NUM_GROUPS, 1), 0, NUM_EXPERTS)
    leading = jnp.arange(GROUP_TOKENS)[None, :] <= CAPACITY
    choice = jnp.where(leading, hot_expert, choice)
    return choice.reshape(TOTAL_TOKENS).astype(jnp.int32)


def expert_weights(key, fan_in, fan_out, weight_scale):
    expert_keys = jax.random.split(key, NUM_EXPERTS)
    return lax.map(lambda one_key: (jax.random.normal(one_key, (fan_in, fan_out), jnp.float32) * weight_scale).astype(jnp.bfloat16), expert_keys)


def setup_inputs(seed: int = 0, part: int = 0) -> dict:
    root_key = jax.random.key(seed)
    key_tokens, key_choice, key_router, key_in, key_out = jax.random.split(root_key, 5)
    tokens = jax.random.normal(jax.random.fold_in(key_tokens, part), (TOTAL_TOKENS, MODEL_DIM), jnp.float32).astype(jnp.bfloat16)
    expert_idx = draw_choices(jax.random.fold_in(key_choice, part))
    w_router = jax.random.normal(key_router, (MODEL_DIM, NUM_EXPERTS), jnp.float32) * MODEL_DIM ** -0.5
    w_in = expert_weights(key_in, MODEL_DIM, HIDDEN_DIM, MODEL_DIM ** -0.5)
    w_out = expert_weights(key_out, HIDDEN_DIM, MODEL_DIM, NUM_EXPERTS * HIDDEN_DIM ** -0.5)
    return {"tokens": tokens, "expert_idx": expert_idx, "w_router": w_router, "w_in": w_in, "w_out": w_out}


def route_group(tok_rows, choice, w_router):
    logits = jnp.dot(tok_rows.astype(jnp.float32), w_router, precision=lax.Precision.HIGHEST)
    router_prob = jax.nn.softmax(logits, axis=-1)
    chosen = choice[:, None] == jnp.arange(NUM_EXPERTS, dtype=jnp.int32)[None, :]
    gate_prob = jnp.sum(jnp.where(chosen, router_prob, 0.0), axis=-1)
    running_count = jnp.cumsum(chosen.astype(jnp.int32), axis=0) - 1
    position = jnp.sum(jnp.where(chosen, running_count, 0), axis=-1)
    slot_index = jnp.where(position < CAPACITY, choice * CAPACITY + position, NUM_EXPERTS * CAPACITY)
    holder = jnp.full((NUM_EXPERTS * CAPACITY + 1,), GROUP_TOKENS, jnp.int32).at[slot_index].set(jnp.arange(GROUP_TOKENS, dtype=jnp.int32))
    buffer = jnp.take(tok_rows, holder[:-1], axis=0, mode="fill", fill_value=0)
    return buffer.reshape(NUM_EXPERTS, CAPACITY, MODEL_DIM), slot_index, gate_prob


def expert_apply(operands):
    rows_in, weight_in, weight_out = operands
    hidden = jnp.dot(rows_in, weight_in, preferred_element_type=jnp.float32)
    hidden_act = jax.nn.relu(hidden).astype(jnp.bfloat16)
    return jnp.dot(hidden_act, weight_out, preferred_element_type=jnp.float32).astype(jnp.bfloat16)


def combine_group(operands):
    flat_out, slot_rows, gate_rows = operands
    picked = jnp.take(flat_out, slot_rows, axis=0, mode="fill", fill_value=0)
    return (gate_rows[:, None] * picked.astype(jnp.float32)).astype(jnp.bfloat16)


def reference(tokens, expert_idx, w_router, w_in, w_out):
    grouped = tokens.reshape(NUM_GROUPS, GROUP_TOKENS, MODEL_DIM)
    choices = expert_idx.reshape(NUM_GROUPS, GROUP_TOKENS)
    buffers, slot_index, gate_prob = lax.map(lambda pair: route_group(pair[0], pair[1], w_router), (grouped, choices))
    per_expert = jnp.swapaxes(buffers, 0, 1).reshape(NUM_EXPERTS, NUM_GROUPS * CAPACITY, MODEL_DIM)
    expert_rows = lax.map(expert_apply, (per_expert, w_in, w_out))
    by_group = jnp.swapaxes(expert_rows.reshape(NUM_EXPERTS, NUM_GROUPS, CAPACITY, MODEL_DIM), 0, 1).reshape(NUM_GROUPS, NUM_EXPERTS * CAPACITY, MODEL_DIM)
    outputs = lax.map(combine_group, (by_group, slot_index, gate_prob))
    return outputs.reshape(TOTAL_TOKENS, MODEL_DIM)
```

```python
import functools

import jax
import jax.numpy as jnp
from jax import lax
from jax.experimental import pallas as pl
from jax.experimental.pallas import tpu as pltpu
from jax.sharding import PartitionSpec as P

MESH = pl.DeviceIdType.MESH
BF16 = jnp.bfloat16
F32 = jnp.float32

TOK = 3072
DIM = 1024
HID = 2816
NEXP = 128
NDEV = 8
LOC = NEXP // NDEV
CAP = 30
ROWS = LOC * CAP
BLK = 256
NBLK = TOK // BLK

HALF = 8 * CAP
D0 = (0, 128)
DN = (128, 112)
R0 = (0, 112)
RN = (112, 128)


def _dot(a, b, **kw):
    return jnp.dot(a, b, preferred_element_type=F32, **kw)


def _kernel(idx_ref, wr_ref, tok_hbm, win_hbm, wout_hbm, y_hbm,
            tok, key, send, recv, ret, win, wout, lhs, hid, meta, stage,
            tok_sem, win_sem, wout_sem, out_sem,
            ds_sem, dr_sem, rs_sem, rr_sem):
    me = lax.axis_index("ep")
    my_c = me % 2
    my_x = (me // 2) % 2
    my_y = me // 4

    def peer(k):
        kc = k % 2
        kx = (k // 2) % 2
        ky = k // 4
        return ((my_y + ky) % 2) * 4 + ((my_x + kx) % 2) * 2 + (my_c + kc) % 2

    tok_copy = pltpu.make_async_copy(tok_hbm, tok, tok_sem)
    tok_copy.start()

    barrier = pltpu.get_barrier_semaphore()
    for k in range(1, NDEV):
        pl.semaphore_signal(barrier, inc=1, device_id={"ep": peer(k)}, device_id_type=MESH)

    def win_copy(e):
        return pltpu.make_async_copy(win_hbm.at[e], win.at[e % 2], win_sem.at[e % 2])

    def wout_copy(e):
        return pltpu.make_async_copy(wout_hbm.at[e], wout.at[e % 2], wout_sem.at[e % 2])

    before = (lax.broadcasted_iota(jnp.int32, (BLK, BLK), 0)
              < lax.broadcasted_iota(jnp.int32, (BLK, BLK), 1)).astype(F32).astype(BF16)
    expert_col = lax.broadcasted_iota(jnp.int32, (NEXP, BLK), 0)
    carry = jnp.zeros((NEXP, 1), F32)
    for b in range(NBLK):
        idx = idx_ref[:, b * BLK:(b + 1) * BLK]
        chosen = jnp.where(expert_col == idx, 1.0, 0.0).astype(F32)
        count = _dot(chosen.astype(BF16), before) + carry
        pos = jnp.sum(chosen * count, axis=0, keepdims=True)
        carry = carry + jnp.sum(chosen, axis=1, keepdims=True)
        slot = idx.astype(F32) * CAP + pos
        key[:, b * BLK:(b + 1) * BLK] = jnp.where(pos < CAP, slot, float(NEXP * CAP))

    tok_copy.wait()
    for e in range(2):
        win_copy(e).start()
        wout_copy(e).start()
    pl.semaphore_wait(barrier, NDEV - 1)

    def d_copy(k, h, j):
        rows = pl.ds(pl.multiple_of(h * HALF + D0[j], 16), DN[j])
        return pltpu.make_async_remote_copy(
            src_ref=send.at[k - 1, rows], dst_ref=recv.at[k, rows],
            send_sem=ds_sem.at[k - 1, h * 2 + j], recv_sem=dr_sem.at[k - 1, h * 2 + j],
            device_id={"ep": peer(k)}, device_id_type=MESH)

    def r_copy(k, h, j):
        rows = pl.ds(pl.multiple_of(h * HALF + R0[j], 16), RN[j])
        return pltpu.make_async_remote_copy(
            src_ref=recv.at[k, rows], dst_ref=ret.at[k - 1, rows],
            send_sem=rs_sem.at[k - 1, h * 2 + j], recv_sem=rr_sem.at[k - 1, h * 2 + j],
            device_id={"ep": peer(k)}, device_id_type=MESH)

    row_id = lax.broadcasted_iota(jnp.int32, (BLK, 1), 0)

    def dispatch(i, _):
        q = i // 4
        p = i % 4
        h = q // 2
        j = q % 2
        first = jnp.where(p == 0, 2, jnp.where(p == 1, 3, jnp.where(p == 2, 6, 0)))
        second = jnp.where(p == 0, 4, jnp.where(p == 1, 5, jnp.where(p == 2, 7, 1)))
        start = pl.multiple_of(h * HALF + j * 128, 16)
        base_a = peer(first) * ROWS + start
        base_b = peer(second) * ROWS + start - 128
        target = (row_id + jnp.where(row_id < 128, base_a, base_b)).astype(F32)
        hid[...] = jnp.where(key[...] == target, 1.0, 0.0).astype(BF16)
        rows = pl.ds(start, 128)
        for n in range(2):
            cols = slice(n * 512, (n + 1) * 512)
            part = _dot(hid[...], tok[:, cols]).astype(BF16)

            @pl.when(p < 3)
            def _():
                send[first - 1, rows, cols] = part[:128]

            @pl.when(p == 3)
            def _():
                recv[0, rows, cols] = part[:128]

            send[second - 1, rows, cols] = part[128:]
        for jj in range(2):
            @pl.when(j == jj)
            def _():
                @pl.when(p < 3)
                def _():
                    d_copy(first, h, jj).start()
                d_copy(second, h, jj).start()
        return 0

    lax.fori_loop(0, 16, dispatch, 0)

    eye = lax.broadcasted_iota(jnp.int32, (BLK, BLK), 0) == lax.broadcasted_iota(jnp.int32, (BLK, BLK), 1)
    lane = lax.broadcasted_iota(jnp.int32, (BLK, NEXP), 1).astype(F32)

    def router(b, _):
        at = pl.ds(pl.multiple_of(b * BLK, BLK), BLK)
        logits = _dot(tok[at, :].astype(F32), wr_ref[...], precision=lax.Precision.HIGHEST)
        top = jnp.max(logits, axis=1, keepdims=True)
        weight = jnp.exp(logits - top)
        total = jnp.sum(weight, axis=1, keepdims=True)
        idx_col = jnp.sum(jnp.where(eye, idx_ref[:, at].astype(F32), 0.0), axis=1, keepdims=True)
        slot_col = jnp.sum(jnp.where(eye, key[:, at], 0.0), axis=1, keepdims=True)
        gate = jnp.sum(jnp.where(lane == idx_col, weight / total, 0.0), axis=1, keepdims=True)
        meta[at, 0:1] = slot_col
        meta[at, 1:2] = gate
        return 0

    lax.fori_loop(0, NBLK, router, 0)

    lhs[...] = jnp.zeros_like(lhs)
    order = (2, 4, 3, 5, 6, 7, 1)

    def group(g, _):
        h = g // 2
        j = g % 2
        for jj in range(2):
            @pl.when(j == jj)
            def _():
                for k in order:
                    d_copy(k, h, jj).wait_recv()

                def spread(k, _):
                    at = pl.ds(pl.multiple_of(k * 32, 32), CAP)
                    block = recv.at[k, pl.ds(pl.multiple_of(h * HALF, 16), HALF)]
                    for c in range(4):
                        lo = (jj * 4 + c) * CAP
                        lhs[c, at, :] = block[lo:lo + CAP, :]
                    return 0

                lax.fori_loop(0, NDEV, spread, 0)

        def expert(c, _):
            e = g * 4 + c
            s = e % 2
            win_copy(e).wait()
            for lo, width in ((0, 768), (768, 768), (1536, 768), (2304, 512)):
                up = _dot(lhs[c], win[s, :, lo:lo + width])
                hid[:, lo:lo + width] = jnp.maximum(up, 0.0).astype(BF16)
            wout_copy(e).wait()
            for n in range(2):
                cols = slice(n * 512, (n + 1) * 512)
                lhs[c, :, cols] = _dot(hid[:, :HID], wout[s, :, cols]).astype(BF16)

            @pl.when(e + 2 < LOC)
            def _():
                win_copy(e + 2).start()
                wout_copy(e + 2).start()
            return 0

        lax.fori_loop(0, 4, expert, 0)

        for jj in range(2):
            @pl.when(j == jj)
            def _():
                def gather(k, _):
                    at = pl.ds(pl.multiple_of(k * 32, 32), CAP)
                    block = recv.at[k, pl.ds(pl.multiple_of(h * HALF, 16), HALF)]
                    for c in range(4):
                        lo = (jj * 4 + c) * CAP
                        block[lo:lo + CAP, :] = lhs[c, at, :]
                    return 0

                lax.fori_loop(0, NDEV, gather, 0)
                for k in order:
                    r_copy(k, h, jj).start()
        return 0

    lax.fori_loop(0, 4, group, 0)

    def combine(peers, lo, n, mode):
        def block(b, _):
            at = pl.ds(pl.multiple_of(b * BLK, BLK), BLK)
            slot = meta[at, 0:1]
            total = None
            for k in peers:
                base = peer(k) * ROWS + lo
                target = (lax.broadcasted_iota(jnp.int32, (1, n), 1) + base).astype(F32)
                pick = jnp.where(slot == target, 1.0, 0.0).astype(BF16)
                rows = recv[0, lo:lo + n, :] if k == 0 else ret[k - 1, lo:lo + n, :]
                part = _dot(pick, rows)
                total = part if total is None else total + part
            if mode != "first":
                total = total + tok[at, :].astype(F32)
            if mode != "last":
                tok[at, :] = total.astype(BF16)
            else:
                s = b % 2

                @pl.when(b >= 2)
                def _():
                    pltpu.make_async_copy(stage.at[s], y_hbm.at[at], out_sem.at[s]).wait()
                stage[s] = (meta[at, 1:2] * total).astype(BF16)
                pltpu.make_async_copy(stage.at[s], y_hbm.at[at], out_sem.at[s]).start()
            return 0

        lax.fori_loop(0, NBLK, block, 0)

    for j in range(2):
        for k in order:
            r_copy(k, 0, j).wait_recv()
    combine((0, 1, 2, 3, 4, 5, 6, 7), 0, HALF, "first")
    for k in order:
        r_copy(k, 1, 0).wait_recv()
    combine((0, 1, 2, 3, 4, 5, 6, 7), HALF, RN[0], "add")
    for k in (1, 2, 4):
        r_copy(k, 1, 1).wait_recv()
    combine((0, 1, 2, 4), HALF + R0[1], RN[1], "add")
    for k in (3, 5):
        r_copy(k, 1, 1).wait_recv()
    combine((3, 5), HALF + R0[1], RN[1], "add")
    for k in (6, 7):
        r_copy(k, 1, 1).wait_recv()
    combine((6, 7), HALF + R0[1], RN[1], "last")

    for h in range(2):
        for j in range(2):
            for k in range(1, NDEV):
                d_copy(k, h, j).wait_send()
                r_copy(k, h, j).wait_send()
    for b in range(NBLK - 2, NBLK):
        at = pl.ds(b * BLK, BLK)
        pltpu.make_async_copy(stage.at[b % 2], y_hbm.at[at], out_sem.at[b % 2]).wait()


def solution(mesh):
    def local_block(tokens, expert_idx, w_router, w_in, w_out):
        any_space = pl.BlockSpec(memory_space=pl.ANY)
        vmem = pl.BlockSpec(memory_space=pltpu.VMEM)
        dma = pltpu.SemaphoreType.DMA
        return pl.pallas_call(
            _kernel,
            out_shape=jax.ShapeDtypeStruct((TOK, DIM), BF16),
            in_specs=[vmem, vmem, any_space, any_space, any_space],
            out_specs=any_space,
            scratch_shapes=[
                pltpu.VMEM((TOK, DIM), BF16),
                pltpu.VMEM((1, TOK), F32),
                pltpu.VMEM((NDEV - 1, ROWS + 16, DIM), BF16),
                pltpu.VMEM((NDEV, ROWS + 16, DIM), BF16),
                pltpu.VMEM((NDEV - 1, ROWS, DIM), BF16),
                pltpu.VMEM((2, DIM, HID), BF16),
                pltpu.VMEM((2, HID, DIM), BF16),
                pltpu.VMEM((4, BLK, DIM), BF16),
                pltpu.VMEM((BLK, TOK), BF16),
                pltpu.VMEM((TOK, 128), F32),
                pltpu.VMEM((2, BLK, DIM), BF16),
                dma, dma((2,)), dma((2,)), dma((2,)),
                dma((NDEV - 1, 4)), dma((NDEV - 1, 4)), dma((NDEV - 1, 4)), dma((NDEV - 1, 4)),
            ],
            compiler_params=pltpu.CompilerParams(
                collective_id=0, has_side_effects=True, vmem_limit_bytes=67043328),
            name="moe_step",
        )(expert_idx.reshape(1, TOK), w_router, tokens, w_in, w_out)

    return jax.shard_map(
        local_block, mesh=mesh,
        in_specs=(P(("dp", "ep"), None), P(("dp", "ep")), P(None, None), P("ep", None, None), P("ep", None, None)),
        out_specs=P(("dp", "ep"), None), check_vma=False)
```

```python
import functools

import jax
import jax.numpy as jnp
from jax import lax
from jax.experimental import pallas as pl
from jax.experimental.pallas import tpu as pltpu
from jax.sharding import PartitionSpec as P

MESH = pl.DeviceIdType.MESH
BF16 = jnp.bfloat16
F32 = jnp.float32

TOK = 3072
DIM = 1024
HID = 2816
NEXP = 128
NDEV = 8
LOC = NEXP // NDEV
CAP = 30
ROWS = LOC * CAP
BLK = 256
NBLK = TOK // BLK

HALF = 8 * CAP
D0 = (0, 128)
DN = (128, 112)
R0 = (0, 112)
RN = (112, 128)


def _dot(a, b, **kw):
    return jnp.dot(a, b, preferred_element_type=F32, **kw)


def _kernel(idx_ref, wr_hbm, tok_hbm, win_hbm, wout_hbm, y_hbm,
            tok, key, send, recv, ret, win, wout, lhs, hid, meta, stage, wr_ref,
            wr_sem, tok_sem, win_sem, wout_sem, out_sem,
            ds_sem, dr_sem, rs_sem, rr_sem):
    me = lax.axis_index("ep")
    my_c = me % 2
    my_x = (me // 2) % 2
    my_y = me // 4

    def peer(k):
        kc = k % 2
        kx = (k // 2) % 2
        ky = k // 4
        return ((my_y + ky) % 2) * 4 + ((my_x + kx) % 2) * 2 + (my_c + kc) % 2

    tok_copy = pltpu.make_async_copy(tok_hbm, tok, tok_sem)
    tok_copy.start()

    barrier = pltpu.get_barrier_semaphore()
    for k in range(1, NDEV):
        pl.semaphore_signal(barrier, inc=1, device_id={"ep": peer(k)}, device_id_type=MESH)

    def win_copy(e):
        return pltpu.make_async_copy(win_hbm.at[e], win.at[e % 2], win_sem.at[e % 2])

    def wout_copy(e):
        return pltpu.make_async_copy(wout_hbm.at[e], wout.at[e % 2], wout_sem.at[e % 2])

    before = (lax.broadcasted_iota(jnp.int32, (BLK, BLK), 0)
              < lax.broadcasted_iota(jnp.int32, (BLK, BLK), 1)).astype(F32).astype(BF16)
    expert_col = lax.broadcasted_iota(jnp.int32, (NEXP, BLK), 0)
    carry = jnp.zeros((NEXP, 1), F32)
    for b in range(NBLK):
        idx = idx_ref[:, b * BLK:(b + 1) * BLK]
        chosen = jnp.where(expert_col == idx, 1.0, 0.0).astype(F32)
        count = _dot(chosen.astype(BF16), before) + carry
        pos = jnp.sum(chosen * count, axis=0, keepdims=True)
        carry = carry + jnp.sum(chosen, axis=1, keepdims=True)
        slot = idx.astype(F32) * CAP + pos
        key[:, b * BLK:(b + 1) * BLK] = jnp.where(pos < CAP, slot, float(NEXP * CAP))

    tok_copy.wait()
    wr_copy = pltpu.make_async_copy(wr_hbm, wr_ref, wr_sem)
    wr_copy.start()
    for e in range(2):
        win_copy(e).start()
        wout_copy(e).start()
    pl.semaphore_wait(barrier, NDEV - 1)

    def d_copy(k, h, j):
        rows = pl.ds(pl.multiple_of(h * HALF + D0[j], 16), DN[j])
        return pltpu.make_async_remote_copy(
            src_ref=send.at[k - 1, rows], dst_ref=recv.at[k, rows],
            send_sem=ds_sem.at[k - 1, h * 2 + j], recv_sem=dr_sem.at[k - 1, h * 2 + j],
            device_id={"ep": peer(k)}, device_id_type=MESH)

    def r_copy(k, h, j):
        rows = pl.ds(pl.multiple_of(h * HALF + R0[j], 16), RN[j])
        return pltpu.make_async_remote_copy(
            src_ref=recv.at[k, rows], dst_ref=ret.at[k - 1, rows],
            send_sem=rs_sem.at[k - 1, h * 2 + j], recv_sem=rr_sem.at[k - 1, h * 2 + j],
            device_id={"ep": peer(k)}, device_id_type=MESH)

    row_id = lax.broadcasted_iota(jnp.int32, (BLK, 1), 0)

    def dispatch(i, _):
        p = jnp.where(i < 8, i % 2, i // 4)
        q = jnp.where(i < 8, i // 2, i % 4)
        h = q // 2
        j = q % 2
        first = jnp.where(p == 0, 2, jnp.where(p == 1, 3, jnp.where(p == 2, 6, 0)))
        second = jnp.where(p == 0, 4, jnp.where(p == 1, 5, jnp.where(p == 2, 7, 1)))
        start = pl.multiple_of(h * HALF + j * 128, 16)
        base_a = peer(first) * ROWS + start
        base_b = peer(second) * ROWS + start - 128
        target = (row_id + jnp.where(row_id < 128, base_a, base_b)).astype(F32)
        hid[...] = jnp.where(key[...] == target, 1.0, 0.0).astype(BF16)
        rows = pl.ds(start, 128)
        for n in range(2):
            cols = slice(n * 512, (n + 1) * 512)
            part = _dot(hid[...], tok[:, cols]).astype(BF16)

            @pl.when(p < 3)
            def _():
                send[first - 1, rows, cols] = part[:128]

            @pl.when(p == 3)
            def _():
                recv[0, rows, cols] = part[:128]

            send[second - 1, rows, cols] = part[128:]
        for jj in range(2):
            @pl.when(j == jj)
            def _():
                @pl.when(p < 3)
                def _():
                    d_copy(first, h, jj).start()
                d_copy(second, h, jj).start()
        return 0

    lax.fori_loop(0, 16, dispatch, 0)

    eye = lax.broadcasted_iota(jnp.int32, (BLK, BLK), 0) == lax.broadcasted_iota(jnp.int32, (BLK, BLK), 1)
    lane = lax.broadcasted_iota(jnp.int32, (BLK, NEXP), 1).astype(F32)

    def router(b, _):
        at = pl.ds(pl.multiple_of(b * BLK, BLK), BLK)
        logits = _dot(tok[at, :].astype(F32), wr_ref[...], precision=lax.Precision.HIGHEST)
        top = jnp.max(logits, axis=1, keepdims=True)
        weight = jnp.exp(logits - top)
        total = jnp.sum(weight, axis=1, keepdims=True)
        idx_col = jnp.sum(jnp.where(eye, idx_ref[:, at].astype(F32), 0.0), axis=1, keepdims=True)
        slot_col = jnp.sum(jnp.where(eye, key[:, at], 0.0), axis=1, keepdims=True)
        gate = jnp.sum(jnp.where(lane == idx_col, weight / total, 0.0), axis=1, keepdims=True)
        meta[at, 0:1] = slot_col
        meta[at, 1:2] = gate
        return 0

    wr_copy.wait()
    lax.fori_loop(0, NBLK, router, 0)

    lhs[...] = jnp.zeros_like(lhs)
    order = (2, 4, 3, 5, 6, 7, 1)

    def group(g, _):
        h = g // 2
        j = g % 2
        for jj in range(2):
            @pl.when(j == jj)
            def _():
                for k in order:
                    d_copy(k, h, jj).wait_recv()

                def spread(k, _):
                    at = pl.ds(pl.multiple_of(k * 32, 32), CAP)
                    block = recv.at[k, pl.ds(pl.multiple_of(h * HALF, 16), HALF)]
                    for c in range(4):
                        lo = (jj * 4 + c) * CAP
                        lhs[c, at, :] = block[lo:lo + CAP, :]
                    return 0

                lax.fori_loop(0, NDEV, spread, 0)

        def expert(c, _):
            e = g * 4 + c
            s = e % 2
            win_copy(e).wait()
            for lo, width in ((0, 768), (768, 768), (1536, 768), (2304, 512)):
                up = _dot(lhs[c], win[s, :, lo:lo + width])
                hid[:, lo:lo + width] = jnp.maximum(up, 0.0).astype(BF16)
            wout_copy(e).wait()
            for n in range(2):
                cols = slice(n * 512, (n + 1) * 512)
                lhs[c, :, cols] = _dot(hid[:, :HID], wout[s, :, cols]).astype(BF16)

            @pl.when(e + 2 < LOC)
            def _():
                win_copy(e + 2).start()
                wout_copy(e + 2).start()
            return 0

        lax.fori_loop(0, 4, expert, 0)

        for jj in range(2):
            @pl.when(j == jj)
            def _():
                def gather(k, _):
                    at = pl.ds(pl.multiple_of(k * 32, 32), CAP)
                    block = recv.at[k, pl.ds(pl.multiple_of(h * HALF, 16), HALF)]
                    for c in range(4):
                        lo = (jj * 4 + c) * CAP
                        block[lo:lo + CAP, :] = lhs[c, at, :]
                    return 0

                lax.fori_loop(0, NDEV, gather, 0)
                for k in (6, 7, 1):
                    r_copy(k, h, jj).start()
        return 0

    lax.fori_loop(0, 4, group, 0)
    for h in range(2):
        for j in range(2):
            for k in (2, 3):
                r_copy(k, h, j).start()

    def combine(peers, lo, n, mode):
        def block(b, _):
            at = pl.ds(pl.multiple_of(b * BLK, BLK), BLK)
            slot = meta[at, 0:1]
            total = None
            for k in peers:
                base = peer(k) * ROWS + lo
                target = (lax.broadcasted_iota(jnp.int32, (1, n), 1) + base).astype(F32)
                pick = jnp.where(slot == target, 1.0, 0.0).astype(BF16)
                rows = recv[0, lo:lo + n, :] if k == 0 else ret[k - 1, lo:lo + n, :]
                part = _dot(pick, rows)
                total = part if total is None else total + part
            if mode != "first":
                total = total + tok[at, :].astype(F32)
            if mode != "last":
                tok[at, :] = total.astype(BF16)
            else:
                s = b % 2

                @pl.when(b >= 2)
                def _():
                    pltpu.make_async_copy(stage.at[s], y_hbm.at[at], out_sem.at[s]).wait()
                stage[s] = (meta[at, 1:2] * total).astype(BF16)
                pltpu.make_async_copy(stage.at[s], y_hbm.at[at], out_sem.at[s]).start()
            return 0

        lax.fori_loop(0, NBLK, block, 0)

    def arrived(peers, *chunks):
        for h, j in chunks:
            for k in peers:
                r_copy(k, h, j).wait_recv()

    arrived((1,), (0, 0), (0, 1), (1, 0), (1, 1))
    combine((0, 1), 0, ROWS, "first")
    arrived((6, 7), (0, 0), (0, 1))
    combine((6, 7), 0, HALF, "add")
    arrived((6, 7), (1, 0), (1, 1))
    for h in range(2):
        for j in range(2):
            for k in (4, 5):
                r_copy(k, h, j).start()
    combine((6, 7), HALF, HALF, "add")
    arrived((2, 3, 4, 5), (0, 0), (0, 1))
    combine((2, 3, 4, 5), 0, HALF, "add")
    arrived((2, 3, 4, 5), (1, 0))
    combine((2, 3, 4, 5), HALF, RN[0], "add")
    arrived((2, 4), (1, 1))
    combine((2, 4), HALF + R0[1], RN[1], "add")
    arrived((3, 5), (1, 1))
    combine((3, 5), HALF + R0[1], RN[1], "last")

    for h in range(2):
        for j in range(2):
            for k in range(1, NDEV):
                d_copy(k, h, j).wait_send()
                r_copy(k, h, j).wait_send()
    for b in range(NBLK - 2, NBLK):
        at = pl.ds(b * BLK, BLK)
        pltpu.make_async_copy(stage.at[b % 2], y_hbm.at[at], out_sem.at[b % 2]).wait()


def solution(mesh):
    def local_block(tokens, expert_idx, w_router, w_in, w_out):
        any_space = pl.BlockSpec(memory_space=pl.ANY)
        vmem = pl.BlockSpec(memory_space=pltpu.VMEM)
        dma = pltpu.SemaphoreType.DMA
        return pl.pallas_call(
            _kernel,
            out_shape=jax.ShapeDtypeStruct((TOK, DIM), BF16),
            in_specs=[vmem, any_space, any_space, any_space, any_space],
            out_specs=any_space,
            scratch_shapes=[
                pltpu.VMEM((TOK, DIM), BF16),
                pltpu.VMEM((1, TOK), F32),
                pltpu.VMEM((NDEV - 1, ROWS + 16, DIM), BF16),
                pltpu.VMEM((NDEV, ROWS + 16, DIM), BF16),
                pltpu.VMEM((NDEV - 1, ROWS, DIM), BF16),
                pltpu.VMEM((2, DIM, HID), BF16),
                pltpu.VMEM((2, HID, DIM), BF16),
                pltpu.VMEM((4, BLK, DIM), BF16),
                pltpu.VMEM((BLK, TOK), BF16),
                pltpu.VMEM((TOK, 128), F32),
                pltpu.VMEM((2, BLK, DIM), BF16),
                pltpu.VMEM((DIM, NEXP), F32),
                dma, dma, dma((2,)), dma((2,)), dma((2,)),
                dma((NDEV - 1, 4)), dma((NDEV - 1, 4)), dma((NDEV - 1, 4)), dma((NDEV - 1, 4)),
            ],
            compiler_params=pltpu.CompilerParams(
                collective_id=0, has_side_effects=True, vmem_limit_bytes=67043328),
            name="moe_step",
        )(expert_idx.reshape(1, TOK), w_router, tokens, w_in, w_out)

    return jax.shard_map(
        local_block, mesh=mesh,
        in_specs=(P(("dp", "ep"), None), P(("dp", "ep")), P(None, None), P("ep", None, None), P("ep", None, None)),
        out_specs=P(("dp", "ep"), None), check_vma=False)
```

```python
import functools

import jax
import jax.numpy as jnp
from jax import lax
from jax.experimental import pallas as pl
from jax.experimental.pallas import tpu as pltpu
from jax.sharding import PartitionSpec as P

MESH = pl.DeviceIdType.MESH
BF16 = jnp.bfloat16
F32 = jnp.float32

TOK = 3072
DIM = 1024
HID = 2816
NEXP = 128
NDEV = 8
LOC = NEXP // NDEV
CAP = 30
ROWS = LOC * CAP
BLK = 256
NBLK = TOK // BLK

HALF = 8 * CAP
D0 = (0, 128)
DN = (128, 112)
R0 = (0, 112)
RN = (112, 128)
LAST = HALF + R0[1]


def _dot(a, b, **kw):
    return jnp.dot(a, b, preferred_element_type=F32, **kw)


def _peer(me, k):
    return (((me // 4 + k // 4) % 2) * 4
            + (((me // 2) % 2 + (k // 2) % 2) % 2) * 2 + (me % 2 + k % 2) % 2)


def _pick(slot, pieces):
    total = None
    for base, rows in pieces:
        target = (lax.broadcasted_iota(jnp.int32, (1, rows.shape[0]), 1) + base).astype(F32)
        part = _dot(jnp.where(slot == target, 1.0, 0.0).astype(BF16), rows[...])
        total = part if total is None else total + part
    return total


def _kernel(idx_ref, wr_hbm, tok_hbm, win_hbm, wout_hbm, y_hbm, meta_hbm, last_hbm,
            tok, key, send, recv, ret, win, wout, lhs, hid, meta, wr_ref,
            wr_sem, tok_sem, y_sem, meta_sem, last_sem, win_sem, wout_sem,
            ds_sem, dr_sem, rs_sem, rr_sem):
    me = lax.axis_index("ep")

    def peer(k):
        return _peer(me, k)

    tok_copy = pltpu.make_async_copy(tok_hbm, tok, tok_sem)
    tok_copy.start()

    barrier = pltpu.get_barrier_semaphore()
    for k in range(1, NDEV):
        pl.semaphore_signal(barrier, inc=1, device_id={"ep": peer(k)}, device_id_type=MESH)

    def win_copy(e):
        return pltpu.make_async_copy(win_hbm.at[e], win.at[e % 2], win_sem.at[e % 2])

    def wout_copy(e):
        return pltpu.make_async_copy(wout_hbm.at[e], wout.at[e % 2], wout_sem.at[e % 2])

    before = (lax.broadcasted_iota(jnp.int32, (BLK, BLK), 0)
              < lax.broadcasted_iota(jnp.int32, (BLK, BLK), 1)).astype(F32).astype(BF16)
    expert_col = lax.broadcasted_iota(jnp.int32, (NEXP, BLK), 0)
    carry = jnp.zeros((NEXP, 1), F32)
    for b in range(NBLK):
        idx = idx_ref[:, b * BLK:(b + 1) * BLK]
        chosen = jnp.where(expert_col == idx, 1.0, 0.0).astype(F32)
        count = _dot(chosen.astype(BF16), before) + carry
        pos = jnp.sum(chosen * count, axis=0, keepdims=True)
        carry = carry + jnp.sum(chosen, axis=1, keepdims=True)
        slot = idx.astype(F32) * CAP + pos
        key[:, b * BLK:(b + 1) * BLK] = jnp.where(pos < CAP, slot, float(NEXP * CAP))

    tok_copy.wait()
    wr_copy = pltpu.make_async_copy(wr_hbm, wr_ref, wr_sem)
    wr_copy.start()
    for e in range(2):
        win_copy(e).start()
        wout_copy(e).start()
    pl.semaphore_wait(barrier, NDEV - 1)

    def d_copy(k, h, j):
        rows = pl.ds(pl.multiple_of(h * HALF + D0[j], 16), DN[j])
        return pltpu.make_async_remote_copy(
            src_ref=send.at[k - 1, rows], dst_ref=recv.at[k, rows],
            send_sem=ds_sem.at[k - 1, h * 2 + j], recv_sem=dr_sem.at[k - 1, h * 2 + j],
            device_id={"ep": peer(k)}, device_id_type=MESH)

    def r_copy(k, h, j):
        rows = pl.ds(pl.multiple_of(h * HALF + R0[j], 16), RN[j])
        return pltpu.make_async_remote_copy(
            src_ref=recv.at[k, rows], dst_ref=ret.at[k - 1, rows],
            send_sem=rs_sem.at[k - 1, h * 2 + j], recv_sem=rr_sem.at[k - 1, h * 2 + j],
            device_id={"ep": peer(k)}, device_id_type=MESH)

    order = (6, 7, 2, 4, 3, 5, 1)
    far = order[:-1]

    row_id = lax.broadcasted_iota(jnp.int32, (BLK, 1), 0)

    def dispatch(i, _):
        q = i // 4
        p = i % 4
        h = q // 2
        j = q % 2
        first = jnp.where(p == 0, 2, jnp.where(p == 1, 3, jnp.where(p == 2, 6, 0)))
        second = jnp.where(p == 0, 4, jnp.where(p == 1, 5, jnp.where(p == 2, 7, 1)))
        start = pl.multiple_of(h * HALF + j * 128, 16)
        base_a = peer(first) * ROWS + start
        base_b = peer(second) * ROWS + start - 128
        target = (row_id + jnp.where(row_id < 128, base_a, base_b)).astype(F32)
        hid[...] = jnp.where(key[...] == target, 1.0, 0.0).astype(BF16)
        rows = pl.ds(start, 128)
        for n in range(2):
            cols = slice(n * 512, (n + 1) * 512)
            part = _dot(hid[...], tok[:, cols]).astype(BF16)

            @pl.when(p < 3)
            def _():
                send[first - 1, rows, cols] = part[:128]

            @pl.when(p == 3)
            def _():
                recv[0, rows, cols] = part[:128]

            send[second - 1, rows, cols] = part[128:]
        for jj in range(2):
            @pl.when(i // 4 == jj)
            def _():
                @pl.when(p < 3)
                def _():
                    d_copy(first, 0, jj).start()
                d_copy(second, 0, jj).start()
        return 0

    lax.fori_loop(0, 16, dispatch, 0)

    eye = lax.broadcasted_iota(jnp.int32, (BLK, BLK), 0) == lax.broadcasted_iota(jnp.int32, (BLK, BLK), 1)
    lane = lax.broadcasted_iota(jnp.int32, (BLK, NEXP), 1).astype(F32)

    def router(b, _):
        at = pl.ds(pl.multiple_of(b * BLK, BLK), BLK)
        logits = _dot(tok[at, :].astype(F32), wr_ref[...], precision=lax.Precision.HIGHEST)
        top = jnp.max(logits, axis=1, keepdims=True)
        weight = jnp.exp(logits - top)
        total = jnp.sum(weight, axis=1, keepdims=True)
        idx_col = jnp.sum(jnp.where(eye, idx_ref[:, at].astype(F32), 0.0), axis=1, keepdims=True)
        slot_col = jnp.sum(jnp.where(eye, key[:, at], 0.0), axis=1, keepdims=True)
        gate = jnp.sum(jnp.where(lane == idx_col, weight / total, 0.0), axis=1, keepdims=True)
        meta[at, 0:1] = slot_col
        meta[at, 1:2] = gate
        return 0

    wr_copy.wait()
    lax.fori_loop(0, NBLK // 2, router, 0)
    for k in order:
        d_copy(k, 1, 0).start()
    lax.fori_loop(NBLK // 2, NBLK, router, 0)
    for k in order:
        d_copy(k, 1, 1).start()

    lhs[...] = jnp.zeros_like(lhs)

    def group(g, _):
        h = g // 2
        j = g % 2
        for jj in range(2):
            @pl.when(j == jj)
            def _():
                for k in order:
                    d_copy(k, h, jj).wait_recv()

                @pl.when(h == 1)
                def _():
                    if jj == 0:
                        for k in far:
                            r_copy(k, 0, 1).start()

                def spread(k, _):
                    at = pl.ds(pl.multiple_of(k * 32, 32), CAP)
                    block = recv.at[k, pl.ds(pl.multiple_of(h * HALF, 16), HALF)]
                    for c in range(4):
                        lo = (jj * 4 + c) * CAP
                        lhs[c, at, :] = block[lo:lo + CAP, :]
                    return 0

                lax.fori_loop(0, NDEV, spread, 0)

        def expert(c, _):
            e = g * 4 + c
            s = e % 2
            win_copy(e).wait()
            for lo, width in ((0, 768), (768, 768), (1536, 768), (2304, 512)):
                up = _dot(lhs[c], win[s, :, lo:lo + width])
                hid[:, lo:lo + width] = jnp.maximum(up, 0.0).astype(BF16)
            wout_copy(e).wait()
            for n in range(2):
                cols = slice(n * 512, (n + 1) * 512)
                lhs[c, :, cols] = _dot(hid[:, :HID], wout[s, :, cols]).astype(BF16)

            @pl.when(e + 2 < LOC)
            def _():
                win_copy(e + 2).start()
                wout_copy(e + 2).start()
            return 0

        lax.fori_loop(0, 4, expert, 0)

        for jj in range(2):
            @pl.when(j == jj)
            def _():
                def gather(k, _):
                    at = pl.ds(pl.multiple_of(k * 32, 32), CAP)
                    block = recv.at[k, pl.ds(pl.multiple_of(h * HALF, 16), HALF)]
                    for c in range(4):
                        lo = (jj * 4 + c) * CAP
                        block[lo:lo + CAP, :] = lhs[c, at, :]
                    return 0

                lax.fori_loop(0, NDEV, gather, 0)
                r_copy(1, h, jj).start()
                if jj == 1:
                    @pl.when(h == 0)
                    def _():
                        for k in far:
                            r_copy(k, 0, 0).start()
        return 0

    lax.fori_loop(0, 4, group, 0)
    for k in far:
        r_copy(k, 1, 0).start()

    def y_copy(b):
        at = pl.ds(pl.multiple_of(b * BLK, BLK), BLK)
        return pltpu.make_async_copy(tok.at[at], y_hbm.at[at], y_sem.at[b])

    def combine(pieces, first=False, last=False):
        def block(b, _):
            if last:
                @pl.when(b >= 1)
                def _():
                    y_copy(b - 1).start()
            at = pl.ds(pl.multiple_of(b * BLK, BLK), BLK)
            total = _pick(meta[at, 0:1], [
                (peer(k) * ROWS + lo, recv.at[0, lo:lo + n] if k == 0 else ret.at[k - 1, lo:lo + n])
                for k, lo, n in pieces])
            if not first:
                total = total + tok[at, :].astype(F32)
            tok[at, :] = total.astype(BF16)
            return 0

        lax.fori_loop(0, NBLK, block, 0)

    def arrived(peers, *chunks):
        for h, j in chunks:
            for k in peers:
                r_copy(k, h, j).wait_recv()

    meta_copy = pltpu.make_async_copy(meta, meta_hbm, meta_sem)
    meta_copy.start()
    arrived((1,), (0, 0), (0, 1), (1, 0), (1, 1))
    combine([(0, 0, ROWS), (1, 0, ROWS)], first=True)
    arrived(far, (0, 0))
    for k in far:
        r_copy(k, 1, 1).start()
    arrived(far, (0, 1))
    combine([(k, 0, HALF) for k in far])
    arrived(far, (1, 0))
    arrived((6, 7), (1, 1))
    combine([(k, HALF, RN[0]) for k in far] + [(k, LAST, RN[1]) for k in (6, 7)], last=True)
    arrived((2, 3, 4, 5), (1, 1))
    y_copy(NBLK - 1).start()
    last_copy = pltpu.make_async_copy(ret.at[1:5, LAST:ROWS], last_hbm, last_sem)
    last_copy.start()

    for h in range(2):
        for j in range(2):
            for k in range(1, NDEV):
                d_copy(k, h, j).wait_send()
                r_copy(k, h, j).wait_send()
    for b in range(NBLK):
        y_copy(b).wait()
    meta_copy.wait()
    last_copy.wait()


def _finish(y_ref, meta_ref, last_ref, out_ref):
    me = lax.axis_index("ep")
    total = _pick(meta_ref[:, 0:1], [(_peer(me, k) * ROWS + LAST, last_ref.at[k - 2]) for k in range(2, 6)])
    total = total + y_ref[...].astype(F32)
    out_ref[...] = (meta_ref[:, 1:2] * total).astype(BF16)


def solution(mesh):
    def local_block(tokens, expert_idx, w_router, w_in, w_out):
        any_space = pl.BlockSpec(memory_space=pl.ANY)
        vmem = pl.BlockSpec(memory_space=pltpu.VMEM)
        dma = pltpu.SemaphoreType.DMA
        partial, meta, last = pl.pallas_call(
            _kernel,
            out_shape=(jax.ShapeDtypeStruct((TOK, DIM), BF16),
                       jax.ShapeDtypeStruct((TOK, 128), F32),
                       jax.ShapeDtypeStruct((4, RN[1], DIM), BF16)),
            in_specs=[vmem, any_space, any_space, any_space, any_space],
            out_specs=(any_space,) * 3,
            scratch_shapes=[
                pltpu.VMEM((TOK, DIM), BF16),
                pltpu.VMEM((1, TOK), F32),
                pltpu.VMEM((NDEV - 1, ROWS + 16, DIM), BF16),
                pltpu.VMEM((NDEV, ROWS + 16, DIM), BF16),
                pltpu.VMEM((NDEV - 1, ROWS, DIM), BF16),
                pltpu.VMEM((2, DIM, HID), BF16),
                pltpu.VMEM((2, HID, DIM), BF16),
                pltpu.VMEM((4, BLK, DIM), BF16),
                pltpu.VMEM((BLK, TOK), BF16),
                pltpu.VMEM((TOK, 128), F32),
                pltpu.VMEM((DIM, NEXP), F32),
                dma, dma, dma((NBLK,)), dma, dma, dma((2,)), dma((2,)),
                dma((NDEV - 1, 4)), dma((NDEV - 1, 4)), dma((NDEV - 1, 4)), dma((NDEV - 1, 4)),
            ],
            compiler_params=pltpu.CompilerParams(
                collective_id=0, has_side_effects=True, vmem_limit_bytes=67043328),
            name="moe_step",
        )(expert_idx.reshape(1, TOK), w_router, tokens, w_in, w_out)
        return pl.pallas_call(
            _finish,
            grid=(NBLK,),
            out_shape=jax.ShapeDtypeStruct((TOK, DIM), BF16),
            in_specs=[pl.BlockSpec((BLK, DIM), lambda b: (b, 0)),
                      pl.BlockSpec((BLK, 128), lambda b: (b, 0)),
                      pl.BlockSpec((4, RN[1], DIM), lambda b: (0, 0, 0))],
            out_specs=pl.BlockSpec((BLK, DIM), lambda b: (b, 0)),
            compiler_params=pltpu.CompilerParams(dimension_semantics=("arbitrary",)),
            name="moe_finish",
        )(partial, meta, last)

    return jax.shard_map(
        local_block, mesh=mesh,
        in_specs=(P(("dp", "ep"), None), P(("dp", "ep")), P(None, None), P("ep", None, None), P("ep", None, None)),
        out_specs=P(("dp", "ep"), None), check_vma=False)
```

```python
import functools

import jax
import jax.numpy as jnp
from jax import lax
from jax.experimental import pallas as pl
from jax.experimental.pallas import tpu as pltpu
from jax.sharding import PartitionSpec as P

MESH = pl.DeviceIdType.MESH
BF16 = jnp.bfloat16
F32 = jnp.float32

TOK = 3072
DIM = 1024
HID = 2816
NEXP = 128
NDEV = 8
LOC = NEXP // NDEV
CAP = 30
ROWS = LOC * CAP
BLK = 256
NBLK = TOK // BLK

HALF = 8 * CAP
D0 = (0, 128)
DN = (128, 112)
R0 = (0, 112)
RN = (112, 128)
LAST = HALF + R0[1]


def _dot(a, b, **kw):
    return jnp.dot(a, b, preferred_element_type=F32, **kw)


def _peer(me, k):
    return (((me // 4 + k // 4) % 2) * 4
            + (((me // 2) % 2 + (k // 2) % 2) % 2) * 2 + (me % 2 + k % 2) % 2)


def _pick(slot, pieces):
    total = None
    for base, rows in pieces:
        target = (lax.broadcasted_iota(jnp.int32, (1, rows.shape[0]), 1) + base).astype(F32)
        part = _dot(jnp.where(slot == target, 1.0, 0.0).astype(BF16), rows[...])
        total = part if total is None else total + part
    return total


def _kernel(idx_ref, wr_hbm, tok_hbm, win_hbm, wout_hbm, y_hbm, meta_hbm, last_hbm,
            tok, key, send, recv, ret, win, wout, lhs, hid, meta, wr_ref,
            wr_sem, tok_sem, y_sem, meta_sem, last_sem, win_sem, wout_sem,
            ds_sem, dr_sem, rs_sem, rr_sem):
    me = lax.axis_index("ep")

    def peer(k):
        return _peer(me, k)

    tok_copy = pltpu.make_async_copy(tok_hbm, tok, tok_sem)
    tok_copy.start()

    barrier = pltpu.get_barrier_semaphore()
    for k in range(1, NDEV):
        pl.semaphore_signal(barrier, inc=1, device_id={"ep": peer(k)}, device_id_type=MESH)

    def win_copy(e):
        return pltpu.make_async_copy(win_hbm.at[e], win.at[e % 2], win_sem.at[e % 2])

    def wout_copy(e):
        return pltpu.make_async_copy(wout_hbm.at[e], wout.at[e % 2], wout_sem.at[e % 2])

    before = (lax.broadcasted_iota(jnp.int32, (BLK, BLK), 0)
              < lax.broadcasted_iota(jnp.int32, (BLK, BLK), 1)).astype(F32).astype(BF16)
    expert_col = lax.broadcasted_iota(jnp.int32, (NEXP, BLK), 0)
    carry = jnp.zeros((NEXP, 1), F32)
    for b in range(NBLK):
        idx = idx_ref[:, b * BLK:(b + 1) * BLK]
        chosen = jnp.where(expert_col == idx, 1.0, 0.0).astype(F32)
        count = _dot(chosen.astype(BF16), before) + carry
        pos = jnp.sum(chosen * count, axis=0, keepdims=True)
        carry = carry + jnp.sum(chosen, axis=1, keepdims=True)
        slot = idx.astype(F32) * CAP + pos
        key[:, b * BLK:(b + 1) * BLK] = jnp.where(pos < CAP, slot, float(NEXP * CAP))

    tok_copy.wait()
    wr_copy = pltpu.make_async_copy(wr_hbm, wr_ref, wr_sem)
    wr_copy.start()
    for e in range(2):
        win_copy(e).start()
        wout_copy(e).start()
    pl.semaphore_wait(barrier, NDEV - 1)

    def d_copy(k, h, j):
        rows = pl.ds(pl.multiple_of(h * HALF + D0[j], 16), DN[j])
        return pltpu.make_async_remote_copy(
            src_ref=send.at[k - 1, rows], dst_ref=recv.at[k, rows],
            send_sem=ds_sem.at[k - 1, h * 2 + j], recv_sem=dr_sem.at[k - 1, h * 2 + j],
            device_id={"ep": peer(k)}, device_id_type=MESH)

    def r_copy(k, h, j):
        rows = pl.ds(pl.multiple_of(h * HALF + R0[j], 16), RN[j])
        return pltpu.make_async_remote_copy(
            src_ref=recv.at[k, rows], dst_ref=ret.at[k - 1, rows],
            send_sem=rs_sem.at[k - 1, h * 2 + j], recv_sem=rr_sem.at[k - 1, h * 2 + j],
            device_id={"ep": peer(k)}, device_id_type=MESH)

    order = (6, 7, 2, 4, 3, 5, 1)
    far = order[:-1]

    row_id = lax.broadcasted_iota(jnp.int32, (BLK, 1), 0)

    def dispatch(i, _):
        q = i // 4
        p = i % 4
        h = q // 2
        j = q % 2
        first = jnp.where(p == 0, 2, jnp.where(p == 1, 3, jnp.where(p == 2, 6, 0)))
        second = jnp.where(p == 0, 4, jnp.where(p == 1, 5, jnp.where(p == 2, 7, 1)))
        start = pl.multiple_of(h * HALF + j * 128, 16)
        base_a = peer(first) * ROWS + start
        base_b = peer(second) * ROWS + start - 128
        target = (row_id + jnp.where(row_id < 128, base_a, base_b)).astype(F32)
        hid[...] = jnp.where(key[...] == target, 1.0, 0.0).astype(BF16)
        rows = pl.ds(start, 128)
        for n in range(2):
            cols = slice(n * 512, (n + 1) * 512)
            part = _dot(hid[...], tok[:, cols]).astype(BF16)

            @pl.when(p < 3)
            def _():
                send[first - 1, rows, cols] = part[:128]

            @pl.when(p == 3)
            def _():
                recv[0, rows, cols] = part[:128]

            send[second - 1, rows, cols] = part[128:]
        for jj in range(2):
            @pl.when(i // 4 == jj)
            def _():
                @pl.when(p < 3)
                def _():
                    d_copy(first, 0, jj).start()
                d_copy(second, 0, jj).start()
        return 0

    lax.fori_loop(0, 16, dispatch, 0)

    eye = lax.broadcasted_iota(jnp.int32, (BLK, BLK), 0) == lax.broadcasted_iota(jnp.int32, (BLK, BLK), 1)
    lane = lax.broadcasted_iota(jnp.int32, (BLK, NEXP), 1).astype(F32)

    def router(b, _):
        at = pl.ds(pl.multiple_of(b * BLK, BLK), BLK)
        logits = _dot(tok[at, :].astype(F32), wr_ref[...], precision=lax.Precision.HIGHEST)
        top = jnp.max(logits, axis=1, keepdims=True)
        weight = jnp.exp(logits - top)
        total = jnp.sum(weight, axis=1, keepdims=True)
        idx_col = jnp.sum(jnp.where(eye, idx_ref[:, at].astype(F32), 0.0), axis=1, keepdims=True)
        slot_col = jnp.sum(jnp.where(eye, key[:, at], 0.0), axis=1, keepdims=True)
        gate = jnp.sum(jnp.where(lane == idx_col, weight / total, 0.0), axis=1, keepdims=True)
        meta[at, 0:1] = slot_col
        meta[at, 1:2] = gate
        return 0

    wr_copy.wait()
    lax.fori_loop(0, NBLK // 2, router, 0)
    for k in order:
        d_copy(k, 1, 0).start()
    lax.fori_loop(NBLK // 2, NBLK, router, 0)
    for k in order:
        d_copy(k, 1, 1).start()

    lhs[...] = jnp.zeros_like(lhs)

    def group(g, _):
        h = g // 2
        j = g % 2
        for jj in range(2):
            @pl.when(j == jj)
            def _():
                for k in order:
                    d_copy(k, h, jj).wait_recv()

                @pl.when(h == 1)
                def _():
                    if jj == 0:
                        for k in far:
                            r_copy(k, 0, 1).start()

                def spread(k, _):
                    at = pl.ds(pl.multiple_of(k * 32, 32), CAP)
                    block = recv.at[k, pl.ds(pl.multiple_of(h * HALF, 16), HALF)]
                    for c in range(4):
                        lo = (jj * 4 + c) * CAP
                        lhs[c, at, :] = block[lo:lo + CAP, :]
                    return 0

                lax.fori_loop(0, NDEV, spread, 0)

        def expert(c, _):
            e = g * 4 + c
            s = e % 2
            win_copy(e).wait()
            for lo, width in ((0, 768), (768, 768), (1536, 768), (2304, 512)):
                up = _dot(lhs[c], win[s, :, lo:lo + width])
                hid[:, lo:lo + width] = jnp.maximum(up, 0.0).astype(BF16)
            wout_copy(e).wait()
            for n in range(2):
                cols = slice(n * 512, (n + 1) * 512)
                lhs[c, :, cols] = _dot(hid[:, :HID], wout[s, :, cols]).astype(BF16)

            @pl.when(e + 2 < LOC)
            def _():
                win_copy(e + 2).start()
                wout_copy(e + 2).start()
            return 0

        lax.fori_loop(0, 4, expert, 0)

        for jj in range(2):
            @pl.when(j == jj)
            def _():
                def gather(k, _):
                    at = pl.ds(pl.multiple_of(k * 32, 32), CAP)
                    block = recv.at[k, pl.ds(pl.multiple_of(h * HALF, 16), HALF)]
                    for c in range(4):
                        lo = (jj * 4 + c) * CAP
                        block[lo:lo + CAP, :] = lhs[c, at, :]
                    return 0

                lax.fori_loop(0, NDEV, gather, 0)
                r_copy(1, h, jj).start()
                if jj == 1:
                    @pl.when(h == 0)
                    def _():
                        for k in far:
                            r_copy(k, 0, 0).start()

                    @pl.when(h == 1)
                    def _():
                        for k in (6, 7):
                            r_copy(k, 1, 1).start()
                else:
                    @pl.when(h == 1)
                    def _():
                        for k in far:
                            r_copy(k, 1, 0).start()
        return 0

    lax.fori_loop(0, 4, group, 0)

    def y_copy(b):
        at = pl.ds(pl.multiple_of(b * BLK, BLK), BLK)
        return pltpu.make_async_copy(tok.at[at], y_hbm.at[at], y_sem.at[b])

    def combine(pieces, first=False, last=False):
        def block(b, _):
            if last:
                @pl.when(b >= 1)
                def _():
                    y_copy(b - 1).start()
            at = pl.ds(pl.multiple_of(b * BLK, BLK), BLK)
            total = _pick(meta[at, 0:1], [
                (peer(k) * ROWS + lo, recv.at[0, lo:lo + n] if k == 0 else ret.at[k - 1, lo:lo + n])
                for k, lo, n in pieces])
            if not first:
                total = total + tok[at, :].astype(F32)
            tok[at, :] = total.astype(BF16)
            return 0

        lax.fori_loop(0, NBLK, block, 0)

    def arrived(peers, *chunks):
        for h, j in chunks:
            for k in peers:
                r_copy(k, h, j).wait_recv()

    meta_copy = pltpu.make_async_copy(meta, meta_hbm, meta_sem)
    meta_copy.start()
    arrived((1,), (0, 0), (0, 1), (1, 0), (1, 1))
    combine([(0, 0, ROWS), (1, 0, ROWS)], first=True)
    arrived(far, (0, 0), (0, 1))
    combine([(k, 0, HALF) for k in far])
    arrived(far, (1, 0))
    for k in (2, 4, 3, 5):
        r_copy(k, 1, 1).start()
    arrived((6, 7), (1, 1))
    combine([(k, HALF, RN[0]) for k in far] + [(k, LAST, RN[1]) for k in (6, 7)], last=True)
    arrived((2, 3, 4, 5), (1, 1))
    y_copy(NBLK - 1).start()
    last_copy = pltpu.make_async_copy(ret.at[1:5, LAST:ROWS], last_hbm, last_sem)
    last_copy.start()

    for h in range(2):
        for j in range(2):
            for k in range(1, NDEV):
                d_copy(k, h, j).wait_send()
                r_copy(k, h, j).wait_send()
    for b in range(NBLK):
        y_copy(b).wait()
    meta_copy.wait()
    last_copy.wait()


def _finish(y_hbm, meta_hbm, last_hbm, out_hbm, y, meta, last, out, y_sem, meta_sem, last_sem, out_sem):
    me = lax.axis_index("ep")

    def rows(b):
        return pl.ds(pl.multiple_of(b * BLK, BLK), BLK)

    def y_copy(b):
        return pltpu.make_async_copy(y_hbm.at[rows(b)], y.at[rows(b)], y_sem.at[b])

    def out_copy(b):
        return pltpu.make_async_copy(out.at[rows(b)], out_hbm.at[rows(b)], out_sem.at[b])

    last_copy = pltpu.make_async_copy(last_hbm, last, last_sem)
    meta_copy = pltpu.make_async_copy(meta_hbm, meta, meta_sem)
    last_copy.start()
    meta_copy.start()
    for b in range(NBLK):
        y_copy(b).start()
    last_copy.wait()
    meta_copy.wait()

    def block(b, _):
        y_copy(b).wait()
        total = _pick(meta[rows(b), 0:1], [(_peer(me, k) * ROWS + LAST, last.at[k - 2]) for k in range(2, 6)])
        total = total + y[rows(b), :].astype(F32)
        out[rows(b), :] = (meta[rows(b), 1:2] * total).astype(BF16)
        out_copy(b).start()
        return 0

    lax.fori_loop(0, NBLK, block, 0)
    for b in range(NBLK):
        out_copy(b).wait()


def solution(mesh):
    def local_block(tokens, expert_idx, w_router, w_in, w_out):
        any_space = pl.BlockSpec(memory_space=pl.ANY)
        vmem = pl.BlockSpec(memory_space=pltpu.VMEM)
        dma = pltpu.SemaphoreType.DMA
        partial, meta, last = pl.pallas_call(
            _kernel,
            out_shape=(jax.ShapeDtypeStruct((TOK, DIM), BF16),
                       jax.ShapeDtypeStruct((TOK, 128), F32),
                       jax.ShapeDtypeStruct((4, RN[1], DIM), BF16)),
            in_specs=[vmem, any_space, any_space, any_space, any_space],
            out_specs=(any_space,) * 3,
            scratch_shapes=[
                pltpu.VMEM((TOK, DIM), BF16),
                pltpu.VMEM((1, TOK), F32),
                pltpu.VMEM((NDEV - 1, ROWS + 16, DIM), BF16),
                pltpu.VMEM((NDEV, ROWS + 16, DIM), BF16),
                pltpu.VMEM((NDEV - 1, ROWS, DIM), BF16),
                pltpu.VMEM((2, DIM, HID), BF16),
                pltpu.VMEM((2, HID, DIM), BF16),
                pltpu.VMEM((4, BLK, DIM), BF16),
                pltpu.VMEM((BLK, TOK), BF16),
                pltpu.VMEM((TOK, 128), F32),
                pltpu.VMEM((DIM, NEXP), F32),
                dma, dma, dma((NBLK,)), dma, dma, dma((2,)), dma((2,)),
                dma((NDEV - 1, 4)), dma((NDEV - 1, 4)), dma((NDEV - 1, 4)), dma((NDEV - 1, 4)),
            ],
            compiler_params=pltpu.CompilerParams(
                collective_id=0, has_side_effects=True, vmem_limit_bytes=67043328),
            name="moe_step",
        )(expert_idx.reshape(1, TOK), w_router, tokens, w_in, w_out)
        return pl.pallas_call(
            _finish,
            out_shape=jax.ShapeDtypeStruct((TOK, DIM), BF16),
            in_specs=[any_space] * 3,
            out_specs=any_space,
            scratch_shapes=[
                pltpu.VMEM((TOK, DIM), BF16),
                pltpu.VMEM((TOK, 128), F32),
                pltpu.VMEM((4, RN[1], DIM), BF16),
                pltpu.VMEM((TOK, DIM), BF16),
                dma((NBLK,)), dma, dma, dma((NBLK,)),
            ],
            compiler_params=pltpu.CompilerParams(vmem_limit_bytes=60 * 2**20),
            name="moe_finish",
        )(partial, meta, last)

    return jax.shard_map(
        local_block, mesh=mesh,
        in_specs=(P(("dp", "ep"), None), P(("dp", "ep")), P(None, None), P("ep", None, None), P("ep", None, None)),
        out_specs=P(("dp", "ep"), None), check_vma=False)
```

```python
import functools

import jax
import jax.numpy as jnp
from jax import lax
from jax.experimental import pallas as pl
from jax.experimental.pallas import tpu as pltpu
from jax.sharding import PartitionSpec as P

MESH = pl.DeviceIdType.MESH
BF16 = jnp.bfloat16
F32 = jnp.float32

TOK = 3072
DIM = 1024
HID = 2816
NEXP = 128
NDEV = 8
LOC = NEXP // NDEV
CAP = 30
ROWS = LOC * CAP
BLK = 256
NBLK = TOK // BLK

HALF = 8 * CAP
D0 = (0, 128)
DN = (128, 112)
R0 = (0, 112)
RN = (112, 128)
LAST = HALF + R0[1]


def _dot(a, b, **kw):
    return jnp.dot(a, b, preferred_element_type=F32, **kw)


def _peer(me, k):
    return (((me // 4 + k // 4) % 2) * 4
            + (((me // 2) % 2 + (k // 2) % 2) % 2) * 2 + (me % 2 + k % 2) % 2)


def _targets(me, pieces):
    width = sum(n for _, _, n in pieces)
    row = lax.broadcasted_iota(jnp.int32, (1, width), 1)
    shift = None
    start = 0
    for k, lo, n in pieces:
        here = _peer(me, k) * ROWS + lo - start
        shift = jnp.full((1, width), here) if shift is None else jnp.where(row >= start, here, shift)
        start += n
    return (row + shift).astype(F32)


def _pick(slot, sources):
    total = None
    for target, rows in sources:
        part = _dot(jnp.where(slot == target, 1.0, 0.0).astype(BF16), rows[...])
        total = part if total is None else total + part
    return total


def _kernel(idx_ref, wr_hbm, tok_hbm, win_hbm, wout_hbm, y_hbm, meta_hbm, last_hbm,
            tok, key, send, recv, ret_p, ret_a, ret_b, ret_c, win, wout, lhs, hid, meta, wr_ref, wr3,
            wr_sem, tok_sem, y_sem, meta_sem, last_sem, win_sem, wout_sem,
            ds_sem, dr_sem, rs_sem, rr_sem):
    me = lax.axis_index("ep")

    def peer(k):
        return _peer(me, k)

    tok_copy = pltpu.make_async_copy(tok_hbm, tok, tok_sem)
    tok_copy.start()

    barrier = pltpu.get_barrier_semaphore()
    for k in range(1, NDEV):
        pl.semaphore_signal(barrier, inc=1, device_id={"ep": peer(k)}, device_id_type=MESH)

    def win_copy(e):
        return pltpu.make_async_copy(win_hbm.at[e], win.at[e % 2], win_sem.at[e % 2])

    def wout_copy(e):
        return pltpu.make_async_copy(wout_hbm.at[e], wout.at[e % 2], wout_sem.at[e % 2])

    before = (lax.broadcasted_iota(jnp.int32, (BLK, BLK), 0)
              < lax.broadcasted_iota(jnp.int32, (BLK, BLK), 1)).astype(F32).astype(BF16)
    expert_col = lax.broadcasted_iota(jnp.int32, (NEXP, BLK), 0)
    carry = jnp.zeros((NEXP, 1), F32)
    for b in range(NBLK):
        idx = idx_ref[:, b * BLK:(b + 1) * BLK]
        chosen = jnp.where(expert_col == idx, 1.0, 0.0).astype(F32)
        count = _dot(chosen.astype(BF16), before) + carry
        pos = jnp.sum(chosen * count, axis=0, keepdims=True)
        carry = carry + jnp.sum(chosen, axis=1, keepdims=True)
        slot = idx.astype(F32) * CAP + pos
        key[:, b * BLK:(b + 1) * BLK] = jnp.where(pos < CAP, slot, float(NEXP * CAP))

    tok_copy.wait()
    wr_copy = pltpu.make_async_copy(wr_hbm, wr_ref, wr_sem)
    wr_copy.start()
    for e in range(2):
        win_copy(e).start()
        wout_copy(e).start()
    pl.semaphore_wait(barrier, NDEV - 1)

    def d_copy(k, h, j):
        rows = pl.ds(pl.multiple_of(h * HALF + D0[j], 16), DN[j])
        return pltpu.make_async_remote_copy(
            src_ref=send.at[k - 1, rows], dst_ref=recv.at[k, rows],
            send_sem=ds_sem.at[k - 1, h * 2 + j], recv_sem=dr_sem.at[k - 1, h * 2 + j],
            device_id={"ep": peer(k)}, device_id_type=MESH)

    def landing(k, h, j):
        if k == 1:
            return ret_p.at[pl.ds(pl.multiple_of(h * HALF + R0[j], 16), RN[j])]
        if h == 0:
            return ret_a.at[pl.ds((k - 2) * HALF + R0[j], RN[j])]
        if j == 0:
            return ret_b.at[pl.ds((k - 2) * RN[0], RN[0])]
        if k >= 6:
            return ret_b.at[pl.ds(6 * RN[0] + (k - 6) * RN[1], RN[1])]
        return ret_c.at[pl.ds((k - 2) * RN[1], RN[1])]

    def r_copy(k, h, j):
        rows = pl.ds(pl.multiple_of(h * HALF + R0[j], 16), RN[j])
        return pltpu.make_async_remote_copy(
            src_ref=recv.at[k, rows], dst_ref=landing(k, h, j),
            send_sem=rs_sem.at[k - 1, h * 2 + j], recv_sem=rr_sem.at[k - 1, h * 2 + j],
            device_id={"ep": peer(k)}, device_id_type=MESH)

    order = (6, 7, 2, 4, 3, 5, 1)
    far = order[:-1]

    row_id = lax.broadcasted_iota(jnp.int32, (BLK, 1), 0)

    def dispatch(i, _):
        q = i // 4
        p = i % 4
        h = q // 2
        j = q % 2
        first = jnp.where(p == 0, 2, jnp.where(p == 1, 3, jnp.where(p == 2, 6, 0)))
        second = jnp.where(p == 0, 4, jnp.where(p == 1, 5, jnp.where(p == 2, 7, 1)))
        start = pl.multiple_of(h * HALF + j * 128, 16)
        base_a = peer(first) * ROWS + start
        base_b = peer(second) * ROWS + start - 128
        target = (row_id + jnp.where(row_id < 128, base_a, base_b)).astype(F32)
        hid[...] = jnp.where(key[...] == target, 1.0, 0.0).astype(BF16)
        rows = pl.ds(start, 128)
        for n in range(2):
            cols = slice(n * 512, (n + 1) * 512)
            part = _dot(hid[...], tok[:, cols]).astype(BF16)

            @pl.when(p < 3)
            def _():
                send[first - 1, rows, cols] = part[:128]

            @pl.when(p == 3)
            def _():
                recv[0, rows, cols] = part[:128]

            send[second - 1, rows, cols] = part[128:]
        @pl.when(i < 4)
        def _():
            @pl.when(p < 3)
            def _():
                d_copy(first, 0, 0).start()
            d_copy(second, 0, 0).start()

        @pl.when(i == 10)
        def _():
            for k in order:
                d_copy(k, 0, 1).start()
        return 0

    lax.fori_loop(0, 16, dispatch, 0)

    eye = lax.broadcasted_iota(jnp.int32, (BLK, BLK), 0) == lax.broadcasted_iota(jnp.int32, (BLK, BLK), 1)
    lane = lax.broadcasted_iota(jnp.int32, (BLK, NEXP), 1).astype(F32)

    def router(b, _):
        at = pl.ds(pl.multiple_of(b * BLK, BLK), BLK)
        parts = _dot(tok[at, :], wr3[...])
        logits = parts[:, :NEXP] + parts[:, NEXP:2 * NEXP] + parts[:, 2 * NEXP:]
        top = jnp.max(logits, axis=1, keepdims=True)
        weight = jnp.exp(logits - top)
        total = jnp.sum(weight, axis=1, keepdims=True)
        idx_col = jnp.sum(jnp.where(eye, idx_ref[:, at].astype(F32), 0.0), axis=1, keepdims=True)
        slot_col = jnp.sum(jnp.where(eye, key[:, at], 0.0), axis=1, keepdims=True)
        gate = jnp.sum(jnp.where(lane == idx_col, weight / total, 0.0), axis=1, keepdims=True)
        meta[at, 0:1] = slot_col
        meta[at, 1:2] = gate
        return 0

    wr_copy.wait()
    top_bf16 = float(jnp.finfo(BF16).max)
    rest = wr_ref[...]
    for n in range(3):
        part = jnp.clip(rest, -top_bf16, top_bf16).astype(BF16)
        wr3[:, n * NEXP:(n + 1) * NEXP] = part
        rest = rest - part.astype(F32)

    lhs[...] = jnp.zeros_like(lhs)

    def group(g, _):
        h = g // 2
        j = g % 2

        @pl.when(g == 2)
        def _():
            lax.fori_loop(0, NBLK, router, 0)

        for jj in range(2):
            @pl.when(j == jj)
            def _():
                for k in order:
                    d_copy(k, h, jj).wait_recv()

                def spread(k, _):
                    at = pl.ds(pl.multiple_of(k * 32, 32), CAP)
                    block = recv.at[k, pl.ds(pl.multiple_of(h * HALF, 16), HALF)]
                    for c in range(4):
                        lo = (jj * 4 + c) * CAP
                        lhs[c, at, :] = block[lo:lo + CAP, :]
                    return 0

                lax.fori_loop(0, NDEV, spread, 0)

        def expert(c, _):
            e = g * 4 + c
            s = e % 2
            win_copy(e).wait()
            for lo, width in ((0, 768), (768, 768), (1536, 768), (2304, 512)):
                up = _dot(lhs[c], win[s, :, lo:lo + width])
                hid[:, lo:lo + width] = jnp.maximum(up, 0.0).astype(BF16)
            wout_copy(e).wait()
            for n in range(2):
                cols = slice(n * 512, (n + 1) * 512)
                lhs[c, :, cols] = _dot(hid[:, :HID], wout[s, :, cols]).astype(BF16)

            @pl.when(e + 2 < LOC)
            def _():
                win_copy(e + 2).start()
                wout_copy(e + 2).start()

            @pl.when(e == 1)
            def _():
                for k in order:
                    d_copy(k, 1, 0).start()

            @pl.when(e == 7)
            def _():
                for k in order:
                    d_copy(k, 1, 1).start()

            @pl.when(e == 10)
            def _():
                for k in far:
                    r_copy(k, 0, 0).start()

            @pl.when(e == 14)
            def _():
                for k in far:
                    r_copy(k, 0, 1).start()
            return 0

        lax.fori_loop(0, 4, expert, 0)

        for jj in range(2):
            @pl.when(j == jj)
            def _():
                def gather(k, _):
                    at = pl.ds(pl.multiple_of(k * 32, 32), CAP)
                    block = recv.at[k, pl.ds(pl.multiple_of(h * HALF, 16), HALF)]
                    for c in range(4):
                        lo = (jj * 4 + c) * CAP
                        block[lo:lo + CAP, :] = lhs[c, at, :]
                    return 0

                lax.fori_loop(0, NDEV, gather, 0)
                r_copy(1, h, jj).start()
        return 0

    lax.fori_loop(0, 4, group, 0)

    def y_copy(b):
        at = pl.ds(pl.multiple_of(b * BLK, BLK), BLK)
        return pltpu.make_async_copy(tok.at[at], y_hbm.at[at], y_sem.at[b])

    def combine(sources, first=False, last=False):
        sources = [(_targets(me, pieces), rows) for pieces, rows in sources]

        def block(b, _):
            if last:
                @pl.when(b >= 1)
                def _():
                    y_copy(b - 1).start()
            at = pl.ds(pl.multiple_of(b * BLK, BLK), BLK)
            total = _pick(meta[at, 0:1], sources)
            if not first:
                total = total + tok[at, :].astype(F32)
            tok[at, :] = total.astype(BF16)
            return 0

        lax.fori_loop(0, NBLK, block, 0)

    def arrived(peers, *chunks):
        for h, j in chunks:
            for k in peers:
                r_copy(k, h, j).wait_recv()

    meta_copy = pltpu.make_async_copy(meta, meta_hbm, meta_sem)
    meta_copy.start()
    arrived((1,), (0, 0), (0, 1), (1, 0), (1, 1))
    combine([([(0, 0, ROWS)], recv.at[0, :ROWS]), ([(1, 0, ROWS)], ret_p)], first=True)
    arrived(far, (0, 0))
    for k in far:
        r_copy(k, 1, 0).start()
    arrived(far, (0, 1))
    for k in (6, 7):
        r_copy(k, 1, 1).start()
    combine([([(k, 0, HALF) for k in range(2, 8)], ret_a)])
    for k in (2, 4, 3, 5):
        r_copy(k, 1, 1).start()
    arrived(far, (1, 0))
    arrived((6, 7), (1, 1))
    combine([([(k, HALF, RN[0]) for k in range(2, 8)] + [(k, LAST, RN[1]) for k in (6, 7)], ret_b)], last=True)
    arrived((2, 3, 4, 5), (1, 1))
    y_copy(NBLK - 1).start()
    last_copy = pltpu.make_async_copy(ret_c, last_hbm, last_sem)
    last_copy.start()

    for h in range(2):
        for j in range(2):
            for k in range(1, NDEV):
                d_copy(k, h, j).wait_send()
                r_copy(k, h, j).wait_send()
    for b in range(NBLK):
        y_copy(b).wait()
    meta_copy.wait()
    last_copy.wait()


def _finish(y_hbm, meta_hbm, last_hbm, out_hbm, y, meta, last, out, y_sem, meta_sem, last_sem, out_sem):
    me = lax.axis_index("ep")

    def rows(b):
        return pl.ds(pl.multiple_of(b * BLK, BLK), BLK)

    def y_copy(b):
        return pltpu.make_async_copy(y_hbm.at[rows(b)], y.at[rows(b)], y_sem.at[b])

    def out_copy(b):
        return pltpu.make_async_copy(out.at[rows(b)], out_hbm.at[rows(b)], out_sem.at[b])

    last_copy = pltpu.make_async_copy(last_hbm, last, last_sem)
    meta_copy = pltpu.make_async_copy(meta_hbm, meta, meta_sem)
    last_copy.start()
    meta_copy.start()
    for b in range(NBLK):
        y_copy(b).start()
    target = _targets(me, [(k, LAST, RN[1]) for k in range(2, 6)])
    last_copy.wait()
    meta_copy.wait()

    def block(b, _):
        y_copy(b).wait()
        total = _pick(meta[rows(b), 0:1], [(target, last)])
        total = total + y[rows(b), :].astype(F32)
        out[rows(b), :] = (meta[rows(b), 1:2] * total).astype(BF16)
        out_copy(b).start()
        return 0

    lax.fori_loop(0, NBLK, block, 0)
    for b in range(NBLK):
        out_copy(b).wait()


def solution(mesh):
    def local_block(tokens, expert_idx, w_router, w_in, w_out):
        any_space = pl.BlockSpec(memory_space=pl.ANY)
        vmem = pl.BlockSpec(memory_space=pltpu.VMEM)
        dma = pltpu.SemaphoreType.DMA
        partial, meta, last = pl.pallas_call(
            _kernel,
            out_shape=(jax.ShapeDtypeStruct((TOK, DIM), BF16),
                       jax.ShapeDtypeStruct((TOK, 128), F32),
                       jax.ShapeDtypeStruct((4 * RN[1], DIM), BF16)),
            in_specs=[vmem, any_space, any_space, any_space, any_space],
            out_specs=(any_space,) * 3,
            scratch_shapes=[
                pltpu.VMEM((TOK, DIM), BF16),
                pltpu.VMEM((1, TOK), F32),
                pltpu.VMEM((NDEV - 1, ROWS + 16, DIM), BF16),
                pltpu.VMEM((NDEV, ROWS + 16, DIM), BF16),
                pltpu.VMEM((ROWS, DIM), BF16),
                pltpu.VMEM((6 * HALF, DIM), BF16),
                pltpu.VMEM((6 * RN[0] + 2 * RN[1], DIM), BF16),
                pltpu.VMEM((4 * RN[1], DIM), BF16),
                pltpu.VMEM((2, DIM, HID), BF16),
                pltpu.VMEM((2, HID, DIM), BF16),
                pltpu.VMEM((4, BLK, DIM), BF16),
                pltpu.VMEM((BLK, TOK), BF16),
                pltpu.VMEM((TOK, 128), F32),
                pltpu.VMEM((DIM, NEXP), F32),
                pltpu.VMEM((DIM, 3 * NEXP), BF16),
                dma, dma, dma((NBLK,)), dma, dma, dma((2,)), dma((2,)),
                dma((NDEV - 1, 4)), dma((NDEV - 1, 4)), dma((NDEV - 1, 4)), dma((NDEV - 1, 4)),
            ],
            compiler_params=pltpu.CompilerParams(
                collective_id=0, has_side_effects=True, vmem_limit_bytes=67043328),
            name="moe_step",
        )(expert_idx.reshape(1, TOK), w_router, tokens, w_in, w_out)
        return pl.pallas_call(
            _finish,
            out_shape=jax.ShapeDtypeStruct((TOK, DIM), BF16),
            in_specs=[any_space] * 3,
            out_specs=any_space,
            scratch_shapes=[
                pltpu.VMEM((TOK, DIM), BF16),
                pltpu.VMEM((TOK, 128), F32),
                pltpu.VMEM((4 * RN[1], DIM), BF16),
                pltpu.VMEM((TOK, DIM), BF16),
                dma((NBLK,)), dma, dma, dma((NBLK,)),
            ],
            compiler_params=pltpu.CompilerParams(vmem_limit_bytes=60 * 2**20),
            name="moe_finish",
        )(partial, meta, last)

    return jax.shard_map(
        local_block, mesh=mesh,
        in_specs=(P(("dp", "ep"), None), P(("dp", "ep")), P(None, None), P("ep", None, None), P("ep", None, None)),
        out_specs=P(("dp", "ep"), None), check_vma=False)
```

```python
import functools

import jax
import jax.numpy as jnp
from jax import lax
from jax.experimental import pallas as pl
from jax.experimental.pallas import tpu as pltpu
from jax.sharding import PartitionSpec as P

MESH = pl.DeviceIdType.MESH
BF16 = jnp.bfloat16
F32 = jnp.float32

TOK = 3072
DIM = 1024
HID = 2816
NEXP = 128
NDEV = 8
LOC = NEXP // NDEV
CAP = 30
ROWS = LOC * CAP
BLK = 256
NBLK = TOK // BLK

HALF = 8 * CAP
D0 = (0, 128)
DN = (128, 112)
R0 = (0, 112)
RN = (112, 128)
LAST = HALF + R0[1]


def _dot(a, b, **kw):
    return jnp.dot(a, b, preferred_element_type=F32, **kw)


def _peer(me, k):
    return (((me // 4 + k // 4) % 2) * 4
            + (((me // 2) % 2 + (k // 2) % 2) % 2) * 2 + (me % 2 + k % 2) % 2)


def _targets(me, pieces):
    width = sum(n for _, _, n in pieces)
    row = lax.broadcasted_iota(jnp.int32, (1, width), 1)
    shift = None
    start = 0
    for k, lo, n in pieces:
        here = _peer(me, k) * ROWS + lo - start
        shift = jnp.full((1, width), here) if shift is None else jnp.where(row >= start, here, shift)
        start += n
    return (row + shift).astype(F32)


def _pick(slot, sources):
    total = None
    for target, rows in sources:
        part = _dot(jnp.where(slot == target, 1.0, 0.0).astype(BF16), rows[...])
        total = part if total is None else total + part
    return total


def _kernel(idx_ref, wr_hbm, tok_hbm, win_hbm, wout_hbm, y_hbm, meta_hbm, last_hbm,
            tok, key, send, recv, ret_p, ret_a, ret_b, ret_c, win, wout, lhs, hid, meta, wr_ref, wr3,
            wr_sem, tok_sem, y_sem, meta_sem, last_sem, win_sem, wout_sem,
            ds_sem, dr_sem, rs_sem, rr_sem):
    me = lax.axis_index("ep")

    def peer(k):
        return _peer(me, k)

    tok_copy = pltpu.make_async_copy(tok_hbm, tok, tok_sem)
    tok_copy.start()

    barrier = pltpu.get_barrier_semaphore()
    for k in range(1, NDEV):
        pl.semaphore_signal(barrier, inc=1, device_id={"ep": peer(k)}, device_id_type=MESH)

    def win_copy(e):
        return pltpu.make_async_copy(win_hbm.at[e], win.at[e % 2], win_sem.at[e % 2])

    def wout_copy(e):
        return pltpu.make_async_copy(wout_hbm.at[e], wout.at[e % 2], wout_sem.at[e % 2])

    before = (lax.broadcasted_iota(jnp.int32, (BLK, BLK), 0)
              < lax.broadcasted_iota(jnp.int32, (BLK, BLK), 1)).astype(F32).astype(BF16)
    expert_col = lax.broadcasted_iota(jnp.int32, (NEXP, BLK), 0)
    carry = jnp.zeros((NEXP, 1), F32)
    for b in range(NBLK):
        idx = idx_ref[:, b * BLK:(b + 1) * BLK]
        chosen = jnp.where(expert_col == idx, 1.0, 0.0).astype(F32)
        count = _dot(chosen.astype(BF16), before) + carry
        pos = jnp.sum(chosen * count, axis=0, keepdims=True)
        carry = carry + jnp.sum(chosen, axis=1, keepdims=True)
        slot = idx.astype(F32) * CAP + pos
        key[:, b * BLK:(b + 1) * BLK] = jnp.where(pos < CAP, slot, float(NEXP * CAP))

    tok_copy.wait()
    wr_copy = pltpu.make_async_copy(wr_hbm, wr_ref, wr_sem)
    wr_copy.start()
    for e in range(2):
        win_copy(e).start()
        wout_copy(e).start()
    pl.semaphore_wait(barrier, NDEV - 1)

    def d_copy(k, h, j):
        rows = pl.ds(pl.multiple_of(h * HALF + D0[j], 16), DN[j])
        return pltpu.make_async_remote_copy(
            src_ref=send.at[k - 1, rows], dst_ref=recv.at[k, rows],
            send_sem=ds_sem.at[k - 1, h * 2 + j], recv_sem=dr_sem.at[k - 1, h * 2 + j],
            device_id={"ep": peer(k)}, device_id_type=MESH)

    def landing(k, h, j):
        if k == 1:
            return ret_p.at[pl.ds(pl.multiple_of(h * HALF + R0[j], 16), RN[j])]
        if h == 0:
            return ret_a.at[pl.ds((k - 2) * HALF + R0[j], RN[j])]
        if j == 0:
            return ret_b.at[pl.ds((k - 2) * RN[0], RN[0])]
        if k >= 6:
            return ret_b.at[pl.ds(6 * RN[0] + (k - 6) * RN[1], RN[1])]
        return ret_c.at[pl.ds((k - 2) * RN[1], RN[1])]

    def r_copy(k, h, j):
        rows = pl.ds(pl.multiple_of(h * HALF + R0[j], 16), RN[j])
        return pltpu.make_async_remote_copy(
            src_ref=recv.at[k, rows], dst_ref=landing(k, h, j),
            send_sem=rs_sem.at[k - 1, h * 2 + j], recv_sem=rr_sem.at[k - 1, h * 2 + j],
            device_id={"ep": peer(k)}, device_id_type=MESH)

    order = (6, 7, 2, 4, 3, 5, 1)
    far = order[:-1]

    row_id = lax.broadcasted_iota(jnp.int32, (BLK, 1), 0)

    def dispatch(i, _):
        q = i // 4
        p = i % 4
        h = q // 2
        j = q % 2
        first = jnp.where(p == 0, 2, jnp.where(p == 1, 3, jnp.where(p == 2, 6, 0)))
        second = jnp.where(p == 0, 4, jnp.where(p == 1, 5, jnp.where(p == 2, 7, 1)))
        start = pl.multiple_of(h * HALF + j * 128, 16)
        base_a = peer(first) * ROWS + start
        base_b = peer(second) * ROWS + start - 128
        target = (row_id + jnp.where(row_id < 128, base_a, base_b)).astype(F32)
        hid[...] = jnp.where(key[...] == target, 1.0, 0.0).astype(BF16)
        rows = pl.ds(start, 128)
        for n in range(2):
            cols = slice(n * 512, (n + 1) * 512)
            part = _dot(hid[...], tok[:, cols]).astype(BF16)

            @pl.when(p < 3)
            def _():
                send[first - 1, rows, cols] = part[:128]

            @pl.when(p == 3)
            def _():
                recv[0, rows, cols] = part[:128]

            send[second - 1, rows, cols] = part[128:]
        @pl.when(i < 4)
        def _():
            @pl.when(p < 3)
            def _():
                d_copy(first, 0, 0).start()
            d_copy(second, 0, 0).start()

        @pl.when(i == 9)
        def _():
            for k in order:
                d_copy(k, 0, 1).start()
        return 0

    lax.fori_loop(0, 16, dispatch, 0)

    eye = lax.broadcasted_iota(jnp.int32, (BLK, BLK), 0) == lax.broadcasted_iota(jnp.int32, (BLK, BLK), 1)
    lane = lax.broadcasted_iota(jnp.int32, (BLK, NEXP), 1).astype(F32)

    def router(b, _):
        at = pl.ds(pl.multiple_of(b * BLK, BLK), BLK)
        parts = _dot(tok[at, :], wr3[...])
        logits = parts[:, :NEXP] + parts[:, NEXP:2 * NEXP] + parts[:, 2 * NEXP:]
        top = jnp.max(logits, axis=1, keepdims=True)
        weight = jnp.exp(logits - top)
        total = jnp.sum(weight, axis=1, keepdims=True)
        idx_col = jnp.sum(jnp.where(eye, idx_ref[:, at].astype(F32), 0.0), axis=1, keepdims=True)
        slot_col = jnp.sum(jnp.where(eye, key[:, at], 0.0), axis=1, keepdims=True)
        gate = jnp.sum(jnp.where(lane == idx_col, weight / total, 0.0), axis=1, keepdims=True)
        meta[at, 0:1] = slot_col
        meta[at, 1:2] = gate
        return 0

    wr_copy.wait()
    top_bf16 = float(jnp.finfo(BF16).max)
    rest = wr_ref[...]
    for n in range(3):
        part = jnp.clip(rest, -top_bf16, top_bf16).astype(BF16)
        wr3[:, n * NEXP:(n + 1) * NEXP] = part
        rest = rest - part.astype(F32)

    lhs[...] = jnp.zeros_like(lhs)

    def group(g, _):
        h = g // 2
        j = g % 2

        @pl.when(g == 2)
        def _():
            lax.fori_loop(0, NBLK, router, 0)

        for jj in range(2):
            @pl.when(j == jj)
            def _():
                for k in order:
                    d_copy(k, h, jj).wait_recv()

                def spread(k, _):
                    at = pl.ds(pl.multiple_of(k * 32, 32), CAP)
                    block = recv.at[k, pl.ds(pl.multiple_of(h * HALF, 16), HALF)]
                    for c in range(4):
                        lo = (jj * 4 + c) * CAP
                        lhs[c, at, :] = block[lo:lo + CAP, :]
                    return 0

                lax.fori_loop(0, NDEV, spread, 0)

        def expert(c, _):
            e = g * 4 + c
            s = e % 2
            win_copy(e).wait()
            for lo, width in ((0, 768), (768, 768), (1536, 768), (2304, 512)):
                up = _dot(lhs[c], win[s, :, lo:lo + width])
                hid[:, lo:lo + width] = jnp.maximum(up, 0.0).astype(BF16)
            wout_copy(e).wait()
            for n in range(2):
                cols = slice(n * 512, (n + 1) * 512)
                lhs[c, :, cols] = _dot(hid[:, :HID], wout[s, :, cols]).astype(BF16)

            @pl.when(e + 2 < LOC)
            def _():
                win_copy(e + 2).start()
                wout_copy(e + 2).start()

            @pl.when(e == 0)
            def _():
                for k in order:
                    d_copy(k, 1, 0).start()

            @pl.when(e == 5)
            def _():
                for k in order:
                    d_copy(k, 1, 1).start()

            @pl.when(e == 9)
            def _():
                for k in far:
                    r_copy(k, 0, 0).start()

            @pl.when(e == 13)
            def _():
                for k in far:
                    r_copy(k, 0, 1).start()
            return 0

        lax.fori_loop(0, 4, expert, 0)

        for jj in range(2):
            @pl.when(j == jj)
            def _():
                def gather(k, _):
                    at = pl.ds(pl.multiple_of(k * 32, 32), CAP)
                    block = recv.at[k, pl.ds(pl.multiple_of(h * HALF, 16), HALF)]
                    for c in range(4):
                        lo = (jj * 4 + c) * CAP
                        block[lo:lo + CAP, :] = lhs[c, at, :]
                    return 0

                lax.fori_loop(0, NDEV, gather, 0)
                r_copy(1, h, jj).start()
        return 0

    lax.fori_loop(0, 4, group, 0)

    def y_copy(b):
        at = pl.ds(pl.multiple_of(b * BLK, BLK), BLK)
        return pltpu.make_async_copy(tok.at[at], y_hbm.at[at], y_sem.at[b])

    def combine(sources, first=False, last=False, midway=None):
        sources = [(_targets(me, pieces), rows) for pieces, rows in sources]

        def block(b, _):
            if last:
                @pl.when(b >= 1)
                def _():
                    y_copy(b - 1).start()
            if midway:
                pl.when(b == 4)(midway)
            at = pl.ds(pl.multiple_of(b * BLK, BLK), BLK)
            total = _pick(meta[at, 0:1], sources)
            if not first:
                total = total + tok[at, :].astype(F32)
            tok[at, :] = total.astype(BF16)
            return 0

        lax.fori_loop(0, NBLK, block, 0, unroll=2)

    def arrived(peers, *chunks):
        for h, j in chunks:
            for k in peers:
                r_copy(k, h, j).wait_recv()

    meta_copy = pltpu.make_async_copy(meta, meta_hbm, meta_sem)
    meta_copy.start()
    arrived((1,), (0, 0), (0, 1), (1, 0), (1, 1))
    combine([([(0, 0, ROWS)], recv.at[0, :ROWS]), ([(1, 0, ROWS)], ret_p)], first=True)
    arrived(far, (0, 0))
    for k in far:
        r_copy(k, 1, 0).start()
    arrived(far, (0, 1))
    for k in (6, 7):
        r_copy(k, 1, 1).start()

    def send_last():
        for k in (2, 4, 3, 5):
            r_copy(k, 1, 1).start()

    combine([([(k, 0, HALF) for k in range(2, 8)], ret_a)], midway=send_last)
    arrived(far, (1, 0))
    arrived((6, 7), (1, 1))
    combine([([(k, HALF, RN[0]) for k in range(2, 8)] + [(k, LAST, RN[1]) for k in (6, 7)], ret_b)], last=True)
    arrived((2, 3, 4, 5), (1, 1))
    y_copy(NBLK - 1).start()
    last_copy = pltpu.make_async_copy(ret_c, last_hbm, last_sem)
    last_copy.start()

    for h in range(2):
        for j in range(2):
            for k in range(1, NDEV):
                d_copy(k, h, j).wait_send()
                r_copy(k, h, j).wait_send()
    for b in range(NBLK):
        y_copy(b).wait()
    meta_copy.wait()
    last_copy.wait()


def _finish(y_hbm, meta_hbm, last_hbm, out_hbm, y, meta, last, out, y_sem, meta_sem, last_sem, out_sem):
    me = lax.axis_index("ep")

    def rows(b):
        return pl.ds(pl.multiple_of(b * BLK, BLK), BLK)

    def y_copy(b):
        return pltpu.make_async_copy(y_hbm.at[rows(b)], y.at[rows(b)], y_sem.at[b])

    def out_copy(b):
        return pltpu.make_async_copy(out.at[rows(b)], out_hbm.at[rows(b)], out_sem.at[b])

    last_copy = pltpu.make_async_copy(last_hbm, last, last_sem)
    meta_copy = pltpu.make_async_copy(meta_hbm, meta, meta_sem)
    last_copy.start()
    meta_copy.start()
    for b in range(NBLK):
        y_copy(b).start()
    target = _targets(me, [(k, LAST, RN[1]) for k in range(2, 6)])
    last_copy.wait()
    meta_copy.wait()

    def block(b, _):
        y_copy(b).wait()
        total = _pick(meta[rows(b), 0:1], [(target, last)])
        total = total + y[rows(b), :].astype(F32)
        out[rows(b), :] = (meta[rows(b), 1:2] * total).astype(BF16)
        out_copy(b).start()
        return 0

    lax.fori_loop(0, NBLK, block, 0, unroll=2)
    for b in range(NBLK):
        out_copy(b).wait()


def solution(mesh):
    def local_block(tokens, expert_idx, w_router, w_in, w_out):
        any_space = pl.BlockSpec(memory_space=pl.ANY)
        vmem = pl.BlockSpec(memory_space=pltpu.VMEM)
        dma = pltpu.SemaphoreType.DMA
        partial, meta, last = pl.pallas_call(
            _kernel,
            out_shape=(jax.ShapeDtypeStruct((TOK, DIM), BF16),
                       jax.ShapeDtypeStruct((TOK, 128), F32),
                       jax.ShapeDtypeStruct((4 * RN[1], DIM), BF16)),
            in_specs=[vmem, any_space, any_space, any_space, any_space],
            out_specs=(any_space,) * 3,
            scratch_shapes=[
                pltpu.VMEM((TOK, DIM), BF16),
                pltpu.VMEM((1, TOK), F32),
                pltpu.VMEM((NDEV - 1, ROWS + 16, DIM), BF16),
                pltpu.VMEM((NDEV, ROWS + 16, DIM), BF16),
                pltpu.VMEM((ROWS, DIM), BF16),
                pltpu.VMEM((6 * HALF, DIM), BF16),
                pltpu.VMEM((6 * RN[0] + 2 * RN[1], DIM), BF16),
                pltpu.VMEM((4 * RN[1], DIM), BF16),
                pltpu.VMEM((2, DIM, HID), BF16),
                pltpu.VMEM((2, HID, DIM), BF16),
                pltpu.VMEM((4, BLK, DIM), BF16),
                pltpu.VMEM((BLK, TOK), BF16),
                pltpu.VMEM((TOK, 128), F32),
                pltpu.VMEM((DIM, NEXP), F32),
                pltpu.VMEM((DIM, 3 * NEXP), BF16),
                dma, dma, dma((NBLK,)), dma, dma, dma((2,)), dma((2,)),
                dma((NDEV - 1, 4)), dma((NDEV - 1, 4)), dma((NDEV - 1, 4)), dma((NDEV - 1, 4)),
            ],
            compiler_params=pltpu.CompilerParams(
                collective_id=0, has_side_effects=True, vmem_limit_bytes=67043328),
            name="moe_step",
        )(expert_idx.reshape(1, TOK), w_router, tokens, w_in, w_out)
        return pl.pallas_call(
            _finish,
            out_shape=jax.ShapeDtypeStruct((TOK, DIM), BF16),
            in_specs=[any_space] * 3,
            out_specs=any_space,
            scratch_shapes=[
                pltpu.VMEM((TOK, DIM), BF16),
                pltpu.VMEM((TOK, 128), F32),
                pltpu.VMEM((4 * RN[1], DIM), BF16),
                pltpu.VMEM((TOK, DIM), BF16),
                dma((NBLK,)), dma, dma, dma((NBLK,)),
            ],
            compiler_params=pltpu.CompilerParams(vmem_limit_bytes=60 * 2**20),
            name="moe_finish",
        )(partial, meta, last)

    return jax.shard_map(
        local_block, mesh=mesh,
        in_specs=(P(("dp", "ep"), None), P(("dp", "ep")), P(None, None), P("ep", None, None), P("ep", None, None)),
        out_specs=P(("dp", "ep"), None), check_vma=False)
```

```python
import functools

import jax
import jax.numpy as jnp
from jax import lax
from jax.experimental import pallas as pl
from jax.experimental.pallas import tpu as pltpu
from jax.sharding import PartitionSpec as P

MESH = pl.DeviceIdType.MESH
BF16 = jnp.bfloat16
F32 = jnp.float32

TOK = 3072
DIM = 1024
HID = 2816
NEXP = 128
NDEV = 8
LOC = NEXP // NDEV
CAP = 30
ROWS = LOC * CAP
BLK = 256
NBLK = TOK // BLK

HALF = 8 * CAP
D0 = (0, 128)
DN = (128, 112)
R0 = (0, 112)
RN = (112, 128)
LAST = HALF + R0[1]


def _dot(a, b, **kw):
    return jnp.dot(a, b, preferred_element_type=F32, **kw)


def _peer(me, k):
    return (((me // 4 + k // 4) % 2) * 4
            + (((me // 2) % 2 + (k // 2) % 2) % 2) * 2 + (me % 2 + k % 2) % 2)


def _targets(me, pieces):
    width = sum(n for _, _, n in pieces)
    row = lax.broadcasted_iota(jnp.int32, (1, width), 1)
    shift = None
    start = 0
    for k, lo, n in pieces:
        here = _peer(me, k) * ROWS + lo - start
        shift = jnp.full((1, width), here) if shift is None else jnp.where(row >= start, here, shift)
        start += n
    return (row + shift).astype(F32)


def _pick(slot, sources):
    total = None
    for target, rows in sources:
        part = _dot(jnp.where(slot == target, 1.0, 0.0).astype(BF16), rows[...])
        total = part if total is None else total + part
    return total


def _kernel(idx_ref, wr_hbm, tok_hbm, win_hbm, wout_hbm, y_hbm, meta_hbm, last_hbm,
            tok, key, send, recv, ret_p, ret_a0, ret_a1, ret_b0, ret_b1, win, wout, lhs, hid, meta, wr_ref, wr3,
            wr_sem, tok_sem, y_sem, meta_sem, win_sem, wout_sem,
            ds_sem, dr_sem, rs_sem, rr_sem):
    me = lax.axis_index("ep")

    def peer(k):
        return _peer(me, k)

    tok_copy = pltpu.make_async_copy(tok_hbm, tok, tok_sem)
    tok_copy.start()

    barrier = pltpu.get_barrier_semaphore()
    for k in range(1, NDEV):
        pl.semaphore_signal(barrier, inc=1, device_id={"ep": peer(k)}, device_id_type=MESH)

    def win_copy(e):
        return pltpu.make_async_copy(win_hbm.at[e], win.at[e % 2], win_sem.at[e % 2])

    def wout_copy(e):
        return pltpu.make_async_copy(wout_hbm.at[e], wout.at[e % 2], wout_sem.at[e % 2])

    before = (lax.broadcasted_iota(jnp.int32, (BLK, BLK), 0)
              < lax.broadcasted_iota(jnp.int32, (BLK, BLK), 1)).astype(F32).astype(BF16)
    expert_col = lax.broadcasted_iota(jnp.int32, (NEXP, BLK), 0)
    carry = jnp.zeros((NEXP, 1), F32)
    for b in range(NBLK):
        idx = idx_ref[:, b * BLK:(b + 1) * BLK]
        chosen = jnp.where(expert_col == idx, 1.0, 0.0).astype(F32)
        count = _dot(chosen.astype(BF16), before) + carry
        pos = jnp.sum(chosen * count, axis=0, keepdims=True)
        carry = carry + jnp.sum(chosen, axis=1, keepdims=True)
        slot = idx.astype(F32) * CAP + pos
        key[:, b * BLK:(b + 1) * BLK] = jnp.where(pos < CAP, slot, float(NEXP * CAP))

    tok_copy.wait()
    wr_copy = pltpu.make_async_copy(wr_hbm, wr_ref, wr_sem)
    wr_copy.start()
    for e in range(2):
        win_copy(e).start()
        wout_copy(e).start()
    pl.semaphore_wait(barrier, NDEV - 1)

    def d_copy(k, h, j):
        rows = pl.ds(pl.multiple_of(h * HALF + D0[j], 16), DN[j])
        return pltpu.make_async_remote_copy(
            src_ref=send.at[k - 1, rows], dst_ref=recv.at[k, rows],
            send_sem=ds_sem.at[k - 1, h * 2 + j], recv_sem=dr_sem.at[k - 1, h * 2 + j],
            device_id={"ep": peer(k)}, device_id_type=MESH)

    def landing(k, h, j):
        if k == 1:
            return ret_p.at[pl.ds(pl.multiple_of(h * HALF + R0[j], 16), RN[j])]
        at = pl.ds((k - 2) * RN[j], RN[j])
        if h == 0:
            return (ret_a0, ret_a1)[j].at[at]
        if j == 0:
            return ret_b0.at[at]
        if k >= 6:
            return ret_b1.at[pl.ds((k - 6) * RN[1], RN[1])]
        return last_hbm.at[at]

    def r_copy(k, h, j):
        rows = pl.ds(pl.multiple_of(h * HALF + R0[j], 16), RN[j])
        return pltpu.make_async_remote_copy(
            src_ref=recv.at[k, rows], dst_ref=landing(k, h, j),
            send_sem=rs_sem.at[k - 1, h * 2 + j], recv_sem=rr_sem.at[k - 1, h * 2 + j],
            device_id={"ep": peer(k)}, device_id_type=MESH)

    order = (6, 7, 2, 4, 3, 5, 1)
    far = order[:-1]

    row_id = lax.broadcasted_iota(jnp.int32, (BLK, 1), 0)

    def dispatch(i, _):
        q = i // 4
        p = i % 4
        h = q // 2
        j = q % 2
        first = jnp.where(p == 0, 2, jnp.where(p == 1, 3, jnp.where(p == 2, 6, 0)))
        second = jnp.where(p == 0, 4, jnp.where(p == 1, 5, jnp.where(p == 2, 7, 1)))
        start = pl.multiple_of(h * HALF + j * 128, 16)
        base_a = peer(first) * ROWS + start
        base_b = peer(second) * ROWS + start - 128
        target = (row_id + jnp.where(row_id < 128, base_a, base_b)).astype(F32)
        hid[...] = jnp.where(key[...] == target, 1.0, 0.0).astype(BF16)
        rows = pl.ds(start, 128)
        for n in range(2):
            cols = slice(n * 512, (n + 1) * 512)
            part = _dot(hid[...], tok[:, cols]).astype(BF16)

            @pl.when(p < 3)
            def _():
                send[first - 1, rows, cols] = part[:128]

            @pl.when(p == 3)
            def _():
                recv[0, rows, cols] = part[:128]

            send[second - 1, rows, cols] = part[128:]
        @pl.when(i < 4)
        def _():
            @pl.when(p < 3)
            def _():
                d_copy(first, 0, 0).start()
            d_copy(second, 0, 0).start()

        @pl.when(i == 9)
        def _():
            for k in order:
                d_copy(k, 0, 1).start()
        return 0

    lax.fori_loop(0, 16, dispatch, 0)

    eye = lax.broadcasted_iota(jnp.int32, (BLK, BLK), 0) == lax.broadcasted_iota(jnp.int32, (BLK, BLK), 1)
    lane = lax.broadcasted_iota(jnp.int32, (BLK, NEXP), 1).astype(F32)

    def router(b, _):
        at = pl.ds(pl.multiple_of(b * BLK, BLK), BLK)
        parts = _dot(tok[at, :], wr3[...])
        logits = parts[:, :NEXP] + parts[:, NEXP:2 * NEXP] + parts[:, 2 * NEXP:]
        top = jnp.max(logits, axis=1, keepdims=True)
        weight = jnp.exp(logits - top)
        total = jnp.sum(weight, axis=1, keepdims=True)
        idx_col = jnp.sum(jnp.where(eye, idx_ref[:, at].astype(F32), 0.0), axis=1, keepdims=True)
        slot_col = jnp.sum(jnp.where(eye, key[:, at], 0.0), axis=1, keepdims=True)
        gate = jnp.sum(jnp.where(lane == idx_col, weight / total, 0.0), axis=1, keepdims=True)
        meta[at, 0:1] = slot_col
        meta[at, 1:2] = gate
        return 0

    wr_copy.wait()
    top_bf16 = float(jnp.finfo(BF16).max)
    rest = wr_ref[...]
    for n in range(3):
        part = jnp.clip(rest, -top_bf16, top_bf16).astype(BF16)
        wr3[:, n * NEXP:(n + 1) * NEXP] = part
        rest = rest - part.astype(F32)

    lhs[...] = jnp.zeros_like(lhs)

    def group(g, _):
        h = g // 2
        j = g % 2

        @pl.when(g == 2)
        def _():
            lax.fori_loop(0, NBLK, router, 0)

        for jj in range(2):
            @pl.when(j == jj)
            def _():
                for k in order:
                    d_copy(k, h, jj).wait_recv()

                def spread(k, _):
                    at = pl.ds(pl.multiple_of(k * 32, 32), CAP)
                    block = recv.at[k, pl.ds(pl.multiple_of(h * HALF, 16), HALF)]
                    for c in range(4):
                        lo = (jj * 4 + c) * CAP
                        lhs[c, at, :] = block[lo:lo + CAP, :]
                    return 0

                lax.fori_loop(0, NDEV, spread, 0)

        def expert(c, _):
            e = g * 4 + c
            s = e % 2
            win_copy(e).wait()
            for lo, width in ((0, 768), (768, 768), (1536, 768), (2304, 512)):
                up = _dot(lhs[c], win[s, :, lo:lo + width])
                hid[:, lo:lo + width] = jnp.maximum(up, 0.0).astype(BF16)
            wout_copy(e).wait()
            for n in range(2):
                cols = slice(n * 512, (n + 1) * 512)
                lhs[c, :, cols] = _dot(hid[:, :HID], wout[s, :, cols]).astype(BF16)

            @pl.when(e + 2 < LOC)
            def _():
                win_copy(e + 2).start()
                wout_copy(e + 2).start()

            @pl.when(e == 1)
            def _():
                for k in order:
                    d_copy(k, 1, 0).start()

            @pl.when(e == 6)
            def _():
                for k in order:
                    d_copy(k, 1, 1).start()

            @pl.when(e == 9)
            def _():
                for k in far:
                    r_copy(k, 0, 0).start()

            @pl.when(e == 15)
            def _():
                for k in far:
                    r_copy(k, 0, 1).start()
            return 0

        lax.fori_loop(0, 4, expert, 0)

        for jj in range(2):
            @pl.when(j == jj)
            def _():
                def gather(k, _):
                    at = pl.ds(pl.multiple_of(k * 32, 32), CAP)
                    block = recv.at[k, pl.ds(pl.multiple_of(h * HALF, 16), HALF)]
                    for c in range(4):
                        lo = (jj * 4 + c) * CAP
                        block[lo:lo + CAP, :] = lhs[c, at, :]
                    return 0

                lax.fori_loop(0, NDEV, gather, 0)
                r_copy(1, h, jj).start()
        return 0

    lax.fori_loop(0, 4, group, 0)

    def y_copy(b):
        at = pl.ds(pl.multiple_of(b * BLK, BLK), BLK)
        return pltpu.make_async_copy(tok.at[at], y_hbm.at[at], y_sem.at[b])

    def combine(sources, first=False, last=False, midway=None):
        sources = [(_targets(me, pieces), rows) for pieces, rows in sources]

        def block(b, _):
            if last:
                @pl.when(b >= 1)
                def _():
                    y_copy(b - 1).start()
            if midway:
                pl.when(b == 8)(midway)
            at = pl.ds(pl.multiple_of(b * BLK, BLK), BLK)
            total = _pick(meta[at, 0:1], sources)
            if not first:
                total = total + tok[at, :].astype(F32)
            tok[at, :] = total.astype(BF16)
            return 0

        lax.fori_loop(0, NBLK, block, 0, unroll=2)

    def arrived(peers, *chunks):
        for h, j in chunks:
            for k in peers:
                r_copy(k, h, j).wait_recv()

    meta_copy = pltpu.make_async_copy(meta, meta_hbm, meta_sem)
    meta_copy.start()
    arrived((1,), (0, 0), (0, 1), (1, 0), (1, 1))
    combine([([(0, 0, ROWS)], recv.at[0, :ROWS]), ([(1, 0, ROWS)], ret_p)], first=True)

    def start(peers, h, j):
        def go():
            for k in peers:
                r_copy(k, h, j).start()
        return go

    arrived(far, (0, 0))
    combine([([(k, R0[0], RN[0]) for k in range(2, 8)], ret_a0)], midway=start(far, 1, 0))
    arrived(far, (0, 1))
    combine([([(k, R0[1], RN[1]) for k in range(2, 8)], ret_a1)], midway=start((6, 7), 1, 1))
    arrived(far, (1, 0))
    start((2, 4, 3, 5), 1, 1)()
    combine([([(k, HALF, RN[0]) for k in range(2, 8)], ret_b0)])
    arrived((6, 7), (1, 1))
    combine([([(k, LAST, RN[1]) for k in (6, 7)], ret_b1)], last=True)
    y_copy(NBLK - 1).start()
    arrived((2, 3, 4, 5), (1, 1))

    for h in range(2):
        for j in range(2):
            for k in range(1, NDEV):
                d_copy(k, h, j).wait_send()
                r_copy(k, h, j).wait_send()
    for b in range(NBLK):
        y_copy(b).wait()
    meta_copy.wait()


def _finish(y_hbm, meta_hbm, last_hbm, out_hbm, y, meta, last, out, y_sem, meta_sem, last_sem, out_sem):
    me = lax.axis_index("ep")

    def rows(b):
        return pl.ds(pl.multiple_of(b * BLK, BLK), BLK)

    def y_copy(b):
        return pltpu.make_async_copy(y_hbm.at[rows(b)], y.at[rows(b)], y_sem.at[b])

    def out_copy(b):
        return pltpu.make_async_copy(out.at[rows(b)], out_hbm.at[rows(b)], out_sem.at[b])

    def meta_copy(b):
        return pltpu.make_async_copy(meta_hbm.at[rows(b)], meta.at[rows(b)], meta_sem.at[b])

    last_copy = pltpu.make_async_copy(last_hbm, last, last_sem)
    last_copy.start()
    for b in range(3):
        meta_copy(b).start()
        y_copy(b).start()
    target = _targets(me, [(k, LAST, RN[1]) for k in range(2, 6)])
    last_copy.wait()

    def block(b, _):
        @pl.when(b + 3 < NBLK)
        def _():
            meta_copy(b + 3).start()
            y_copy(b + 3).start()
        meta_copy(b).wait()
        y_copy(b).wait()
        total = _pick(meta[rows(b), 0:1], [(target, last)])
        total = total + y[rows(b), :].astype(F32)
        out[rows(b), :] = (meta[rows(b), 1:2] * total).astype(BF16)
        out_copy(b).start()
        return 0

    lax.fori_loop(0, NBLK, block, 0)
    for b in range(NBLK):
        out_copy(b).wait()


def solution(mesh):
    def local_block(tokens, expert_idx, w_router, w_in, w_out):
        any_space = pl.BlockSpec(memory_space=pl.ANY)
        vmem = pl.BlockSpec(memory_space=pltpu.VMEM)
        dma = pltpu.SemaphoreType.DMA
        partial, meta, last = pl.pallas_call(
            _kernel,
            out_shape=(jax.ShapeDtypeStruct((TOK, DIM), BF16),
                       jax.ShapeDtypeStruct((TOK, 128), F32),
                       jax.ShapeDtypeStruct((4 * RN[1], DIM), BF16)),
            in_specs=[vmem, any_space, any_space, any_space, any_space],
            out_specs=(any_space,) * 3,
            scratch_shapes=[
                pltpu.VMEM((TOK, DIM), BF16),
                pltpu.VMEM((1, TOK), F32),
                pltpu.VMEM((NDEV - 1, ROWS + 16, DIM), BF16),
                pltpu.VMEM((NDEV, ROWS + 16, DIM), BF16),
                pltpu.VMEM((ROWS, DIM), BF16),
                pltpu.VMEM((6 * RN[0], DIM), BF16),
                pltpu.VMEM((6 * RN[1], DIM), BF16),
                pltpu.VMEM((6 * RN[0], DIM), BF16),
                pltpu.VMEM((2 * RN[1], DIM), BF16),
                pltpu.VMEM((2, DIM, HID), BF16),
                pltpu.VMEM((2, HID, DIM), BF16),
                pltpu.VMEM((4, BLK, DIM), BF16),
                pltpu.VMEM((BLK, TOK), BF16),
                pltpu.VMEM((TOK, 128), F32),
                pltpu.VMEM((DIM, NEXP), F32),
                pltpu.VMEM((DIM, 3 * NEXP), BF16),
                dma, dma, dma((NBLK,)), dma, dma((2,)), dma((2,)),
                dma((NDEV - 1, 4)), dma((NDEV - 1, 4)), dma((NDEV - 1, 4)), dma((NDEV - 1, 4)),
            ],
            compiler_params=pltpu.CompilerParams(
                collective_id=0, has_side_effects=True, vmem_limit_bytes=67043328),
            name="moe_step",
        )(expert_idx.reshape(1, TOK), w_router, tokens, w_in, w_out)
        return pl.pallas_call(
            _finish,
            out_shape=jax.ShapeDtypeStruct((TOK, DIM), BF16),
            in_specs=[any_space] * 3,
            out_specs=any_space,
            scratch_shapes=[
                pltpu.VMEM((TOK, DIM), BF16),
                pltpu.VMEM((TOK, 128), F32),
                pltpu.VMEM((4 * RN[1], DIM), BF16),
                pltpu.VMEM((TOK, DIM), BF16),
                dma((NBLK,)), dma((NBLK,)), dma, dma((NBLK,)),
            ],
            compiler_params=pltpu.CompilerParams(vmem_limit_bytes=60 * 2**20),
            name="moe_finish",
        )(partial, meta, last)

    return jax.shard_map(
        local_block, mesh=mesh,
        in_specs=(P(("dp", "ep"), None), P(("dp", "ep")), P(None, None), P("ep", None, None), P("ep", None, None)),
        out_specs=P(("dp", "ep"), None), check_vma=False)
```

```python
import functools

import jax
import jax.numpy as jnp
from jax import lax
from jax.experimental import pallas as pl
from jax.experimental.pallas import tpu as pltpu
from jax.sharding import PartitionSpec as P

MESH = pl.DeviceIdType.MESH
BF16 = jnp.bfloat16
F32 = jnp.float32

TOK = 3072
DIM = 1024
HID = 2816
NEXP = 128
NDEV = 8
LOC = NEXP // NDEV
CAP = 30
ROWS = LOC * CAP
BLK = 256
NBLK = TOK // BLK

HALF = 8 * CAP
D0 = (0, 128)
DN = (128, 112)
R0 = (0, 112)
RN = (112, 128)
LAST = HALF + R0[1]


def _dot(a, b, **kw):
    return jnp.dot(a, b, preferred_element_type=F32, **kw)


def _peer(me, k):
    return (((me // 4 + k // 4) % 2) * 4
            + (((me // 2) % 2 + (k // 2) % 2) % 2) * 2 + (me % 2 + k % 2) % 2)


def _targets(me, pieces):
    width = sum(n for _, _, n in pieces)
    row = lax.broadcasted_iota(jnp.int32, (1, width), 1)
    shift = None
    start = 0
    for k, lo, n in pieces:
        here = _peer(me, k) * ROWS + lo - start
        shift = jnp.full((1, width), here) if shift is None else jnp.where(row >= start, here, shift)
        start += n
    return (row + shift).astype(F32)


def _pick(slot, sources):
    total = None
    for target, rows in sources:
        part = _dot(jnp.where(slot == target, 1.0, 0.0).astype(BF16), rows[...])
        total = part if total is None else total + part
    return total


def _kernel(idx_ref, wr_hbm, tok_hbm, win_hbm, wout_hbm, y_hbm, meta_hbm, last_hbm,
            tok, key, send, recv, ret_p, ret_a0, ret_a1, ret_b0, ret_b1, win, wout, lhs, hid, meta, wr_ref, wr3,
            wr_sem, tok_sem, y_sem, meta_sem, win_sem, wout_sem,
            ds_sem, dr_sem, rs_sem, rr_sem):
    me = lax.axis_index("ep")

    def peer(k):
        return _peer(me, k)

    tok_copy = pltpu.make_async_copy(tok_hbm, tok, tok_sem)
    tok_copy.start()

    barrier = pltpu.get_barrier_semaphore()
    for k in range(1, NDEV):
        pl.semaphore_signal(barrier, inc=1, device_id={"ep": peer(k)}, device_id_type=MESH)

    def win_copy(e):
        return pltpu.make_async_copy(win_hbm.at[e], win.at[e % 2], win_sem.at[e % 2])

    def wout_copy(e):
        return pltpu.make_async_copy(wout_hbm.at[e], wout.at[e % 2], wout_sem.at[e % 2])

    before = (lax.broadcasted_iota(jnp.int32, (BLK, BLK), 0)
              < lax.broadcasted_iota(jnp.int32, (BLK, BLK), 1)).astype(F32).astype(BF16)
    expert_col = lax.broadcasted_iota(jnp.int32, (NEXP, BLK), 0)
    carry = jnp.zeros((NEXP, 1), F32)
    for b in range(NBLK):
        idx = idx_ref[:, b * BLK:(b + 1) * BLK]
        chosen = jnp.where(expert_col == idx, 1.0, 0.0).astype(F32)
        count = _dot(chosen.astype(BF16), before) + carry
        pos = jnp.sum(chosen * count, axis=0, keepdims=True)
        carry = carry + jnp.sum(chosen, axis=1, keepdims=True)
        slot = idx.astype(F32) * CAP + pos
        key[:, b * BLK:(b + 1) * BLK] = jnp.where(pos < CAP, slot, float(NEXP * CAP))

    tok_copy.wait()
    wr_copy = pltpu.make_async_copy(wr_hbm, wr_ref, wr_sem)
    wr_copy.start()
    for e in range(2):
        win_copy(e).start()
        wout_copy(e).start()

    def d_copy(k, h, j):
        rows = pl.ds(pl.multiple_of(h * HALF + D0[j], 16), DN[j])
        return pltpu.make_async_remote_copy(
            src_ref=send.at[k - 1, rows], dst_ref=recv.at[k, rows],
            send_sem=ds_sem.at[k - 1, h * 2 + j], recv_sem=dr_sem.at[k - 1, h * 2 + j],
            device_id={"ep": peer(k)}, device_id_type=MESH)

    def landing(k, h, j):
        if k == 1:
            return ret_p.at[pl.ds(pl.multiple_of(h * HALF + R0[j], 16), RN[j])]
        at = pl.ds((k - 2) * RN[j], RN[j])
        if h == 0:
            return (ret_a0, ret_a1)[j].at[at]
        if j == 0:
            return ret_b0.at[at]
        if k >= 6:
            return ret_b1.at[pl.ds((k - 6) * RN[1], RN[1])]
        return last_hbm.at[at]

    def r_copy(k, h, j):
        rows = pl.ds(pl.multiple_of(h * HALF + R0[j], 16), RN[j])
        return pltpu.make_async_remote_copy(
            src_ref=recv.at[k, rows], dst_ref=landing(k, h, j),
            send_sem=rs_sem.at[k - 1, h * 2 + j], recv_sem=rr_sem.at[k - 1, h * 2 + j],
            device_id={"ep": peer(k)}, device_id_type=MESH)

    order = (6, 7, 2, 4, 3, 5, 1)
    far = order[:-1]

    row_id = lax.broadcasted_iota(jnp.int32, (BLK, 1), 0)

    def dispatch(i, _):
        q = i // 4
        p = i % 4
        h = q // 2
        j = q % 2
        first = jnp.where(p == 0, 2, jnp.where(p == 1, 3, jnp.where(p == 2, 6, 0)))
        second = jnp.where(p == 0, 4, jnp.where(p == 1, 5, jnp.where(p == 2, 7, 1)))
        start = pl.multiple_of(h * HALF + j * 128, 16)
        base_a = peer(first) * ROWS + start
        base_b = peer(second) * ROWS + start - 128
        target = (row_id + jnp.where(row_id < 128, base_a, base_b)).astype(F32)
        hid[...] = jnp.where(key[...] == target, 1.0, 0.0).astype(BF16)
        rows = pl.ds(start, 128)
        for n in range(2):
            cols = slice(n * 512, (n + 1) * 512)
            part = _dot(hid[...], tok[:, cols]).astype(BF16)

            @pl.when(p < 3)
            def _():
                send[first - 1, rows, cols] = part[:128]

            @pl.when(p == 3)
            def _():
                recv[0, rows, cols] = part[:128]

            send[second - 1, rows, cols] = part[128:]
        @pl.when(i == 0)
        def _():
            pl.semaphore_wait(barrier, NDEV - 1)

        @pl.when(i < 4)
        def _():
            @pl.when(p < 3)
            def _():
                d_copy(first, 0, 0).start()
            d_copy(second, 0, 0).start()

        @pl.when(i == 9)
        def _():
            for k in order:
                d_copy(k, 0, 1).start()
        return 0

    lax.fori_loop(0, 16, dispatch, 0)

    eye = lax.broadcasted_iota(jnp.int32, (BLK, BLK), 0) == lax.broadcasted_iota(jnp.int32, (BLK, BLK), 1)
    lane = lax.broadcasted_iota(jnp.int32, (BLK, NEXP), 1).astype(F32)

    def router(b, _):
        at = pl.ds(pl.multiple_of(b * BLK, BLK), BLK)
        parts = _dot(tok[at, :], wr3[...])
        logits = parts[:, :NEXP] + parts[:, NEXP:2 * NEXP] + parts[:, 2 * NEXP:]
        top = jnp.max(logits, axis=1, keepdims=True)
        weight = jnp.exp(logits - top)
        total = jnp.sum(weight, axis=1, keepdims=True)
        idx_col = jnp.sum(jnp.where(eye, idx_ref[:, at].astype(F32), 0.0), axis=1, keepdims=True)
        slot_col = jnp.sum(jnp.where(eye, key[:, at], 0.0), axis=1, keepdims=True)
        gate = jnp.sum(jnp.where(lane == idx_col, weight / total, 0.0), axis=1, keepdims=True)
        meta[at, 0:1] = slot_col
        meta[at, 1:2] = gate
        return 0

    wr_copy.wait()
    top_bf16 = float(jnp.finfo(BF16).max)
    rest = wr_ref[...]
    for n in range(3):
        part = jnp.clip(rest, -top_bf16, top_bf16).astype(BF16)
        wr3[:, n * NEXP:(n + 1) * NEXP] = part
        rest = rest - part.astype(F32)

    lhs[...] = jnp.zeros_like(lhs)

    def group(g, _):
        h = g // 2
        j = g % 2

        @pl.when(g == 2)
        def _():
            lax.fori_loop(0, NBLK, router, 0)

        for jj in range(2):
            @pl.when(j == jj)
            def _():
                for k in order:
                    d_copy(k, h, jj).wait_recv()

                def spread(k, _):
                    at = pl.ds(pl.multiple_of(k * 32, 32), CAP)
                    block = recv.at[k, pl.ds(pl.multiple_of(h * HALF, 16), HALF)]
                    for c in range(4):
                        lo = (jj * 4 + c) * CAP
                        lhs[c, at, :] = block[lo:lo + CAP, :]
                    return 0

                lax.fori_loop(0, NDEV, spread, 0)

        def expert(c, _):
            e = g * 4 + c
            s = e % 2
            win_copy(e).wait()
            for lo, width in ((0, 768), (768, 768), (1536, 768), (2304, 512)):
                up = _dot(lhs[c], win[s, :, lo:lo + width])
                hid[:, lo:lo + width] = jnp.maximum(up, 0.0).astype(BF16)
            wout_copy(e).wait()
            for n in range(2):
                cols = slice(n * 512, (n + 1) * 512)
                lhs[c, :, cols] = _dot(hid[:, :HID], wout[s, :, cols]).astype(BF16)

            @pl.when(e + 2 < LOC)
            def _():
                win_copy(e + 2).start()
                wout_copy(e + 2).start()

            @pl.when(e == 1)
            def _():
                for k in order:
                    d_copy(k, 1, 0).start()

            @pl.when(e == 6)
            def _():
                for k in order:
                    d_copy(k, 1, 1).start()

            @pl.when(e == 9)
            def _():
                for k in far:
                    r_copy(k, 0, 0).start()

            @pl.when(e == 15)
            def _():
                for k in far:
                    r_copy(k, 0, 1).start()
            return 0

        lax.fori_loop(0, 4, expert, 0)

        for jj in range(2):
            @pl.when(j == jj)
            def _():
                def gather(k, _):
                    at = pl.ds(pl.multiple_of(k * 32, 32), CAP)
                    block = recv.at[k, pl.ds(pl.multiple_of(h * HALF, 16), HALF)]
                    for c in range(4):
                        lo = (jj * 4 + c) * CAP
                        block[lo:lo + CAP, :] = lhs[c, at, :]
                    return 0

                lax.fori_loop(0, NDEV, gather, 0)
                r_copy(1, h, jj).start()
        return 0

    lax.fori_loop(0, 4, group, 0)

    def y_copy(b):
        at = pl.ds(pl.multiple_of(b * BLK, BLK), BLK)
        return pltpu.make_async_copy(tok.at[at], y_hbm.at[at], y_sem.at[b])

    def combine(sources, first=False, last=False, midway=None):
        sources = [(_targets(me, pieces), rows) for pieces, rows in sources]

        def block(b, _):
            if last:
                @pl.when(b >= 1)
                def _():
                    y_copy(b - 1).start()
            if midway:
                pl.when(b == 8)(midway)
            at = pl.ds(pl.multiple_of(b * BLK, BLK), BLK)
            total = _pick(meta[at, 0:1], sources)
            if not first:
                total = total + tok[at, :].astype(F32)
            tok[at, :] = total.astype(BF16)
            return 0

        lax.fori_loop(0, NBLK, block, 0, unroll=2)

    def arrived(peers, *chunks):
        for h, j in chunks:
            for k in peers:
                r_copy(k, h, j).wait_recv()

    meta_copy = pltpu.make_async_copy(meta, meta_hbm, meta_sem)
    meta_copy.start()
    arrived((1,), (0, 0), (0, 1), (1, 0), (1, 1))
    combine([([(0, 0, ROWS)], recv.at[0, :ROWS]), ([(1, 0, ROWS)], ret_p)], first=True)

    def start(peers, h, j):
        def go():
            for k in peers:
                r_copy(k, h, j).start()
        return go

    arrived(far, (0, 0))
    combine([([(k, R0[0], RN[0]) for k in range(2, 8)], ret_a0)], midway=start(far, 1, 0))
    arrived(far, (0, 1))
    combine([([(k, R0[1], RN[1]) for k in range(2, 8)], ret_a1)], midway=start((6, 7), 1, 1))
    arrived(far, (1, 0))
    start((2, 4, 3, 5), 1, 1)()
    combine([([(k, HALF, RN[0]) for k in range(2, 8)], ret_b0)])
    arrived((6, 7), (1, 1))
    combine([([(k, LAST, RN[1]) for k in (6, 7)], ret_b1)], last=True)
    y_copy(NBLK - 1).start()
    arrived((2, 3, 4, 5), (1, 1))

    for h in range(2):
        for j in range(2):
            for k in range(1, NDEV):
                d_copy(k, h, j).wait_send()
                r_copy(k, h, j).wait_send()
    for b in range(NBLK):
        y_copy(b).wait()
    meta_copy.wait()


def _finish(y_hbm, meta_hbm, last_hbm, out_hbm, y, meta, last, out, y_sem, meta_sem, last_sem, out_sem):
    me = lax.axis_index("ep")

    def rows(b):
        return pl.ds(pl.multiple_of(b * BLK, BLK), BLK)

    def y_copy(b):
        return pltpu.make_async_copy(y_hbm.at[rows(b)], y.at[rows(b)], y_sem.at[b])

    def out_copy(b):
        return pltpu.make_async_copy(out.at[rows(b)], out_hbm.at[rows(b)], out_sem.at[b])

    def meta_copy(b):
        return pltpu.make_async_copy(meta_hbm.at[rows(b)], meta.at[rows(b)], meta_sem.at[b])

    last_copy = pltpu.make_async_copy(last_hbm, last, last_sem)
    last_copy.start()
    for b in range(3):
        meta_copy(b).start()
        y_copy(b).start()
    target = _targets(me, [(k, LAST, RN[1]) for k in range(2, 6)])
    last_copy.wait()

    def block(b, _):
        @pl.when(b + 3 < NBLK)
        def _():
            meta_copy(b + 3).start()
            y_copy(b + 3).start()
        meta_copy(b).wait()
        y_copy(b).wait()
        total = _pick(meta[rows(b), 0:1], [(target, last)])
        total = total + y[rows(b), :].astype(F32)
        out[rows(b), :] = (meta[rows(b), 1:2] * total).astype(BF16)
        out_copy(b).start()
        return 0

    lax.fori_loop(0, NBLK, block, 0, unroll=2)
    for b in range(NBLK):
        out_copy(b).wait()


def solution(mesh):
    def local_block(tokens, expert_idx, w_router, w_in, w_out):
        any_space = pl.BlockSpec(memory_space=pl.ANY)
        vmem = pl.BlockSpec(memory_space=pltpu.VMEM)
        dma = pltpu.SemaphoreType.DMA
        partial, meta, last = pl.pallas_call(
            _kernel,
            out_shape=(jax.ShapeDtypeStruct((TOK, DIM), BF16),
                       jax.ShapeDtypeStruct((TOK, 128), F32),
                       jax.ShapeDtypeStruct((4 * RN[1], DIM), BF16)),
            in_specs=[vmem, any_space, any_space, any_space, any_space],
            out_specs=(any_space,) * 3,
            scratch_shapes=[
                pltpu.VMEM((TOK, DIM), BF16),
                pltpu.VMEM((1, TOK), F32),
                pltpu.VMEM((NDEV - 1, ROWS + 16, DIM), BF16),
                pltpu.VMEM((NDEV, ROWS + 16, DIM), BF16),
                pltpu.VMEM((ROWS, DIM), BF16),
                pltpu.VMEM((6 * RN[0], DIM), BF16),
                pltpu.VMEM((6 * RN[1], DIM), BF16),
                pltpu.VMEM((6 * RN[0], DIM), BF16),
                pltpu.VMEM((2 * RN[1], DIM), BF16),
                pltpu.VMEM((2, DIM, HID), BF16),
                pltpu.VMEM((2, HID, DIM), BF16),
                pltpu.VMEM((4, BLK, DIM), BF16),
                pltpu.VMEM((BLK, TOK), BF16),
                pltpu.VMEM((TOK, 128), F32),
                pltpu.VMEM((DIM, NEXP), F32),
                pltpu.VMEM((DIM, 3 * NEXP), BF16),
                dma, dma, dma((NBLK,)), dma, dma((2,)), dma((2,)),
                dma((NDEV - 1, 4)), dma((NDEV - 1, 4)), dma((NDEV - 1, 4)), dma((NDEV - 1, 4)),
            ],
            compiler_params=pltpu.CompilerParams(
                collective_id=0, has_side_effects=True, vmem_limit_bytes=67043328),
            name="moe_step",
        )(expert_idx.reshape(1, TOK), w_router, tokens, w_in, w_out)
        return pl.pallas_call(
            _finish,
            out_shape=jax.ShapeDtypeStruct((TOK, DIM), BF16),
            in_specs=[any_space] * 3,
            out_specs=any_space,
            scratch_shapes=[
                pltpu.VMEM((TOK, DIM), BF16),
                pltpu.VMEM((TOK, 128), F32),
                pltpu.VMEM((4 * RN[1], DIM), BF16),
                pltpu.VMEM((TOK, DIM), BF16),
                dma((NBLK,)), dma((NBLK,)), dma, dma((NBLK,)),
            ],
            compiler_params=pltpu.CompilerParams(vmem_limit_bytes=60 * 2**20),
            name="moe_finish",
        )(partial, meta, last)

    return jax.shard_map(
        local_block, mesh=mesh,
        in_specs=(P(("dp", "ep"), None), P(("dp", "ep")), P(None, None), P("ep", None, None), P("ep", None, None)),
        out_specs=P(("dp", "ep"), None), check_vma=False)
```

```python
import functools

import jax
import jax.numpy as jnp
from jax import lax
from jax.experimental import pallas as pl
from jax.experimental.pallas import tpu as pltpu
from jax.sharding import PartitionSpec as P

MESH = pl.DeviceIdType.MESH
BF16 = jnp.bfloat16
F32 = jnp.float32

TOK = 3072
DIM = 1024
HID = 2816
NEXP = 128
NDEV = 8
LOC = NEXP // NDEV
CAP = 30
ROWS = LOC * CAP
BLK = 256
NBLK = TOK // BLK

HALF = 8 * CAP
D0 = (0, 128)
DN = (128, 112)
R0 = (0, 112)
RN = (112, 128)
LAST = HALF + R0[1]


def _dot(a, b, **kw):
    return jnp.dot(a, b, preferred_element_type=F32, **kw)


def _peer(me, k):
    return (((me // 4 + k // 4) % 2) * 4
            + (((me // 2) % 2 + (k // 2) % 2) % 2) * 2 + (me % 2 + k % 2) % 2)


def _targets(me, pieces):
    width = sum(n for _, _, n in pieces)
    row = lax.broadcasted_iota(jnp.int32, (1, width), 1)
    shift = None
    start = 0
    for k, lo, n in pieces:
        here = _peer(me, k) * ROWS + lo - start
        shift = jnp.full((1, width), here) if shift is None else jnp.where(row >= start, here, shift)
        start += n
    return (row + shift).astype(F32)


def _pick(slot, sources):
    total = None
    for target, rows in sources:
        part = _dot(jnp.where(slot == target, 1.0, 0.0).astype(BF16), rows[...])
        total = part if total is None else total + part
    return total


def _kernel(idx_ref, wr_hbm, tok_hbm, win_hbm, wout_hbm, y_hbm, meta_hbm, last_hbm,
            tok, key, send, recv, ret_p, ret_a0, ret_a1, ret_b0, ret_b1, win, wout, lhs, hid, meta, wr_ref, wr3,
            wr_sem, tok_sem, y_sem, meta_sem, win_sem, wout_sem,
            ds_sem, dr_sem, rs_sem, rr_sem):
    me = lax.axis_index("ep")

    def peer(k):
        return _peer(me, k)

    tok_copy = pltpu.make_async_copy(tok_hbm, tok, tok_sem)
    tok_copy.start()

    barrier = pltpu.get_barrier_semaphore()
    for k in range(1, NDEV):
        pl.semaphore_signal(barrier, inc=1, device_id={"ep": peer(k)}, device_id_type=MESH)

    def win_copy(e):
        return pltpu.make_async_copy(win_hbm.at[e], win.at[e % 2], win_sem.at[e % 2])

    def wout_copy(e):
        return pltpu.make_async_copy(wout_hbm.at[e], wout.at[e % 2], wout_sem.at[e % 2])

    before = (lax.broadcasted_iota(jnp.int32, (BLK, BLK), 0)
              < lax.broadcasted_iota(jnp.int32, (BLK, BLK), 1)).astype(F32).astype(BF16)
    expert_col = lax.broadcasted_iota(jnp.int32, (NEXP, BLK), 0)
    carry = jnp.zeros((NEXP, 1), F32)
    for b in range(NBLK):
        idx = idx_ref[:, b * BLK:(b + 1) * BLK]
        chosen = jnp.where(expert_col == idx, 1.0, 0.0).astype(F32)
        count = _dot(chosen.astype(BF16), before) + carry
        pos = jnp.sum(chosen * count, axis=0, keepdims=True)
        carry = carry + jnp.sum(chosen, axis=1, keepdims=True)
        slot = idx.astype(F32) * CAP + pos
        key[:, b * BLK:(b + 1) * BLK] = jnp.where(pos < CAP, slot, float(NEXP * CAP))

    tok_copy.wait()
    wr_copy = pltpu.make_async_copy(wr_hbm, wr_ref, wr_sem)
    wr_copy.start()
    for e in range(2):
        win_copy(e).start()
        wout_copy(e).start()

    def d_copy(k, h, j):
        rows = pl.ds(pl.multiple_of(h * HALF + D0[j], 16), DN[j])
        return pltpu.make_async_remote_copy(
            src_ref=send.at[k - 1, rows], dst_ref=recv.at[k, rows],
            send_sem=ds_sem.at[k - 1, h * 2 + j], recv_sem=dr_sem.at[k - 1, h * 2 + j],
            device_id={"ep": peer(k)}, device_id_type=MESH)

    def landing(k, h, j):
        if k == 1:
            return ret_p.at[pl.ds(pl.multiple_of(h * HALF + R0[j], 16), RN[j])]
        at = pl.ds((k - 2) * RN[j], RN[j])
        if h == 0:
            return (ret_a0, ret_a1)[j].at[at]
        if j == 0:
            return ret_b0.at[at]
        if k >= 6:
            return ret_b1.at[pl.ds((k - 6) * RN[1], RN[1])]
        return last_hbm.at[at]

    def r_copy(k, h, j):
        rows = pl.ds(pl.multiple_of(h * HALF + R0[j], 16), RN[j])
        return pltpu.make_async_remote_copy(
            src_ref=recv.at[k, rows], dst_ref=landing(k, h, j),
            send_sem=rs_sem.at[k - 1, h * 2 + j], recv_sem=rr_sem.at[k - 1, h * 2 + j],
            device_id={"ep": peer(k)}, device_id_type=MESH)

    order = (6, 7, 2, 4, 3, 5, 1)
    far = order[:-1]

    row_id = lax.broadcasted_iota(jnp.int32, (BLK, 1), 0)

    def dispatch(i, _):
        q = i // 4
        p = i % 4
        h = q // 2
        j = q % 2
        first = jnp.where(p == 0, 2, jnp.where(p == 1, 3, jnp.where(p == 2, 6, 0)))
        second = jnp.where(p == 0, 4, jnp.where(p == 1, 5, jnp.where(p == 2, 7, 1)))
        start = pl.multiple_of(h * HALF + j * 128, 16)
        base_a = peer(first) * ROWS + start
        base_b = peer(second) * ROWS + start - 128
        target = (row_id + jnp.where(row_id < 128, base_a, base_b)).astype(F32)
        hid[...] = jnp.where(key[...] == target, 1.0, 0.0).astype(BF16)
        rows = pl.ds(start, 128)
        for n in range(2):
            cols = slice(n * 512, (n + 1) * 512)
            part = _dot(hid[...], tok[:, cols]).astype(BF16)

            @pl.when(p < 3)
            def _():
                send[first - 1, rows, cols] = part[:128]

            @pl.when(p == 3)
            def _():
                recv[0, rows, cols] = part[:128]

            send[second - 1, rows, cols] = part[128:]
        @pl.when(i == 0)
        def _():
            pl.semaphore_wait(barrier, NDEV - 1)

        @pl.when(i < 4)
        def _():
            @pl.when(p < 3)
            def _():
                d_copy(first, 0, 0).start()
            d_copy(second, 0, 0).start()

        @pl.when(i == 9)
        def _():
            for k in order:
                d_copy(k, 0, 1).start()
        return 0

    lax.fori_loop(0, 16, dispatch, 0)

    eye = lax.broadcasted_iota(jnp.int32, (BLK, BLK), 0) == lax.broadcasted_iota(jnp.int32, (BLK, BLK), 1)
    lane = lax.broadcasted_iota(jnp.int32, (BLK, NEXP), 1).astype(F32)

    def router(b, _):
        at = pl.ds(pl.multiple_of(b * BLK, BLK), BLK)
        parts = _dot(tok[at, :], wr3[...])
        logits = parts[:, :NEXP] + parts[:, NEXP:2 * NEXP] + parts[:, 2 * NEXP:]
        top = jnp.max(logits, axis=1, keepdims=True)
        weight = jnp.exp(logits - top)
        total = jnp.sum(weight, axis=1, keepdims=True)
        idx_col = jnp.sum(jnp.where(eye, idx_ref[:, at].astype(F32), 0.0), axis=1, keepdims=True)
        slot_col = jnp.sum(jnp.where(eye, key[:, at], 0.0), axis=1, keepdims=True)
        gate = jnp.sum(jnp.where(lane == idx_col, weight / total, 0.0), axis=1, keepdims=True)
        meta[at, 0:1] = slot_col
        meta[at, 1:2] = gate
        return 0

    wr_copy.wait()
    top_bf16 = float(jnp.finfo(BF16).max)
    rest = wr_ref[...]
    for n in range(3):
        part = jnp.clip(rest, -top_bf16, top_bf16).astype(BF16)
        wr3[:, n * NEXP:(n + 1) * NEXP] = part
        rest = rest - part.astype(F32)

    lhs[...] = jnp.zeros_like(lhs)

    def group(g, _):
        h = g // 2
        j = g % 2

        @pl.when(g == 2)
        def _():
            lax.fori_loop(0, NBLK, router, 0)

        for jj in range(2):
            @pl.when(j == jj)
            def _():
                for k in order:
                    d_copy(k, h, jj).wait_recv()

                def spread(k, _):
                    at = pl.ds(pl.multiple_of(k * 32, 32), CAP)
                    block = recv.at[k, pl.ds(pl.multiple_of(h * HALF, 16), HALF)]
                    for c in range(4):
                        lo = (jj * 4 + c) * CAP
                        lhs[c, at, :] = block[lo:lo + CAP, :]
                    return 0

                lax.fori_loop(0, NDEV, spread, 0)

        def expert(c, _):
            e = g * 4 + c
            s = e % 2
            win_copy(e).wait()
            for lo, width in ((0, 768), (768, 768), (1536, 768), (2304, 512)):
                up = _dot(lhs[c], win[s, :, lo:lo + width])
                hid[:, lo:lo + width] = jnp.maximum(up, 0.0).astype(BF16)
            wout_copy(e).wait()
            for n in range(2):
                cols = slice(n * 512, (n + 1) * 512)
                lhs[c, :, cols] = _dot(hid[:, :HID], wout[s, :, cols]).astype(BF16)

            @pl.when(e + 2 < LOC)
            def _():
                win_copy(e + 2).start()
                wout_copy(e + 2).start()

            @pl.when(e == 1)
            def _():
                for k in order:
                    d_copy(k, 1, 0).start()

            @pl.when(e == 6)
            def _():
                for k in order:
                    d_copy(k, 1, 1).start()

            @pl.when(e == 9)
            def _():
                for k in far:
                    r_copy(k, 0, 0).start()

            @pl.when(e == 15)
            def _():
                for k in far:
                    r_copy(k, 0, 1).start()
            return 0

        lax.fori_loop(0, 4, expert, 0)

        for jj in range(2):
            @pl.when(j == jj)
            def _():
                def gather(k, _):
                    at = pl.ds(pl.multiple_of(k * 32, 32), CAP)
                    block = recv.at[k, pl.ds(pl.multiple_of(h * HALF, 16), HALF)]
                    for c in range(4):
                        lo = (jj * 4 + c) * CAP
                        block[lo:lo + CAP, :] = lhs[c, at, :]
                    return 0

                lax.fori_loop(0, NDEV, gather, 0)
                r_copy(1, h, jj).start()
        return 0

    lax.fori_loop(0, 4, group, 0)

    def y_copy(b):
        at = pl.ds(pl.multiple_of(b * BLK, BLK), BLK)
        return pltpu.make_async_copy(tok.at[at], y_hbm.at[at], y_sem.at[b])

    def combine(sources, first=False, last=False, midway=None, when=0):
        sources = [(_targets(me, pieces), rows) for pieces, rows in sources]

        def block(b, _):
            if last:
                @pl.when(b >= 1)
                def _():
                    y_copy(b - 1).start()
            if midway:
                pl.when(b == when)(midway)
            at = pl.ds(pl.multiple_of(b * BLK, BLK), BLK)
            total = _pick(meta[at, 0:1], sources)
            if not first:
                total = total + tok[at, :].astype(F32)
            tok[at, :] = total.astype(BF16)
            return 0

        lax.fori_loop(0, NBLK, block, 0, unroll=2)

    def arrived(peers, *chunks):
        for h, j in chunks:
            for k in peers:
                r_copy(k, h, j).wait_recv()

    meta_copy = pltpu.make_async_copy(meta, meta_hbm, meta_sem)
    meta_copy.start()
    arrived((1,), (0, 0), (0, 1), (1, 0), (1, 1))
    combine([([(0, 0, ROWS)], recv.at[0, :ROWS]), ([(1, 0, ROWS)], ret_p)], first=True)

    def start(peers, h, j):
        def go():
            for k in peers:
                r_copy(k, h, j).start()
        return go

    arrived(far, (0, 0))
    combine([([(k, R0[0], RN[0]) for k in range(2, 8)], ret_a0)], midway=start(far, 1, 0), when=11)
    arrived(far, (0, 1))
    combine([([(k, R0[1], RN[1]) for k in range(2, 8)], ret_a1)], midway=start((6, 7), 1, 1), when=2)
    arrived(far, (1, 0))
    start((2, 4, 3, 5), 1, 1)()
    combine([([(k, HALF, RN[0]) for k in range(2, 8)], ret_b0)])
    arrived((6, 7), (1, 1))
    combine([([(k, LAST, RN[1]) for k in (6, 7)], ret_b1)], last=True)
    y_copy(NBLK - 1).start()
    arrived((2, 3, 4, 5), (1, 1))

    for h in range(2):
        for j in range(2):
            for k in range(1, NDEV):
                d_copy(k, h, j).wait_send()
                r_copy(k, h, j).wait_send()
    for b in range(NBLK):
        y_copy(b).wait()
    meta_copy.wait()


def _finish(y_hbm, meta_hbm, last_hbm, out_hbm, y, meta, last, out, y_sem, meta_sem, last_sem, out_sem):
    me = lax.axis_index("ep")

    def rows(b):
        return pl.ds(pl.multiple_of(b * BLK, BLK), BLK)

    def y_copy(b):
        return pltpu.make_async_copy(y_hbm.at[rows(b)], y.at[rows(b)], y_sem.at[b])

    def out_copy(b):
        return pltpu.make_async_copy(out.at[rows(b)], out_hbm.at[rows(b)], out_sem.at[b])

    def meta_copy(b):
        return pltpu.make_async_copy(meta_hbm.at[rows(b)], meta.at[rows(b)], meta_sem.at[b])

    last_copy = pltpu.make_async_copy(last_hbm, last, last_sem)
    last_copy.start()
    for b in range(5):
        meta_copy(b).start()
        y_copy(b).start()
    target = _targets(me, [(k, LAST, RN[1]) for k in range(2, 6)])
    last_copy.wait()

    def block(b, _):
        @pl.when(b + 5 < NBLK)
        def _():
            meta_copy(b + 5).start()
            y_copy(b + 5).start()
        meta_copy(b).wait()
        y_copy(b).wait()
        total = _pick(meta[rows(b), 0:1], [(target, last)])
        total = total + y[rows(b), :].astype(F32)
        out[rows(b), :] = (meta[rows(b), 1:2] * total).astype(BF16)
        out_copy(b).start()
        return 0

    lax.fori_loop(0, NBLK, block, 0, unroll=2)
    for b in range(NBLK):
        out_copy(b).wait()


def solution(mesh):
    def local_block(tokens, expert_idx, w_router, w_in, w_out):
        any_space = pl.BlockSpec(memory_space=pl.ANY)
        vmem = pl.BlockSpec(memory_space=pltpu.VMEM)
        dma = pltpu.SemaphoreType.DMA
        partial, meta, last = pl.pallas_call(
            _kernel,
            out_shape=(jax.ShapeDtypeStruct((TOK, DIM), BF16),
                       jax.ShapeDtypeStruct((TOK, 128), F32),
                       jax.ShapeDtypeStruct((4 * RN[1], DIM), BF16)),
            in_specs=[vmem, any_space, any_space, any_space, any_space],
            out_specs=(any_space,) * 3,
            scratch_shapes=[
                pltpu.VMEM((TOK, DIM), BF16),
                pltpu.VMEM((1, TOK), F32),
                pltpu.VMEM((NDEV - 1, ROWS + 16, DIM), BF16),
                pltpu.VMEM((NDEV, ROWS + 16, DIM), BF16),
                pltpu.VMEM((ROWS, DIM), BF16),
                pltpu.VMEM((6 * RN[0], DIM), BF16),
                pltpu.VMEM((6 * RN[1], DIM), BF16),
                pltpu.VMEM((6 * RN[0], DIM), BF16),
                pltpu.VMEM((2 * RN[1], DIM), BF16),
                pltpu.VMEM((2, DIM, HID), BF16),
                pltpu.VMEM((2, HID, DIM), BF16),
                pltpu.VMEM((4, BLK, DIM), BF16),
                pltpu.VMEM((BLK, TOK), BF16),
                pltpu.VMEM((TOK, 128), F32),
                pltpu.VMEM((DIM, NEXP), F32),
                pltpu.VMEM((DIM, 3 * NEXP), BF16),
                dma, dma, dma((NBLK,)), dma, dma((2,)), dma((2,)),
                dma((NDEV - 1, 4)), dma((NDEV - 1, 4)), dma((NDEV - 1, 4)), dma((NDEV - 1, 4)),
            ],
            compiler_params=pltpu.CompilerParams(
                collective_id=0, has_side_effects=True, vmem_limit_bytes=67043328),
            name="moe_step",
        )(expert_idx.reshape(1, TOK), w_router, tokens, w_in, w_out)
        return pl.pallas_call(
            _finish,
            out_shape=jax.ShapeDtypeStruct((TOK, DIM), BF16),
            in_specs=[any_space] * 3,
            out_specs=any_space,
            scratch_shapes=[
                pltpu.VMEM((TOK, DIM), BF16),
                pltpu.VMEM((TOK, 128), F32),
                pltpu.VMEM((4 * RN[1], DIM), BF16),
                pltpu.VMEM((TOK, DIM), BF16),
                dma((NBLK,)), dma((NBLK,)), dma, dma((NBLK,)),
            ],
            compiler_params=pltpu.CompilerParams(vmem_limit_bytes=60 * 2**20),
            name="moe_finish",
        )(partial, meta, last)

    return jax.shard_map(
        local_block, mesh=mesh,
        in_specs=(P(("dp", "ep"), None), P(("dp", "ep")), P(None, None), P("ep", None, None), P("ep", None, None)),
        out_specs=P(("dp", "ep"), None), check_vma=False)
```

```python
import functools

import jax
import jax.numpy as jnp
from jax import lax
from jax.experimental import pallas as pl
from jax.experimental.pallas import tpu as pltpu
from jax.sharding import PartitionSpec as P

MESH = pl.DeviceIdType.MESH
BF16 = jnp.bfloat16
F32 = jnp.float32

TOK = 3072
DIM = 1024
HID = 2816
NEXP = 128
NDEV = 8
LOC = NEXP // NDEV
CAP = 30
ROWS = LOC * CAP
BLK = 256
NBLK = TOK // BLK

HALF = 8 * CAP
D0 = (0, 128)
DN = (128, 112)
R0 = (0, 112)
RN = (112, 128)
LAST = HALF + R0[1]


def _dot(a, b, **kw):
    return jnp.dot(a, b, preferred_element_type=F32, **kw)


def _peer(me, k):
    return (((me // 4 + k // 4) % 2) * 4
            + (((me // 2) % 2 + (k // 2) % 2) % 2) * 2 + (me % 2 + k % 2) % 2)


def _targets(me, pieces):
    width = sum(n for _, _, n in pieces)
    row = lax.broadcasted_iota(jnp.int32, (1, width), 1)
    shift = None
    start = 0
    for k, lo, n in pieces:
        here = _peer(me, k) * ROWS + lo - start
        shift = jnp.full((1, width), here) if shift is None else jnp.where(row >= start, here, shift)
        start += n
    return (row + shift).astype(F32)


def _pick(slot, sources):
    total = None
    for target, rows in sources:
        part = _dot(jnp.where(slot == target, 1.0, 0.0).astype(BF16), rows[...])
        total = part if total is None else total + part
    return total


def _kernel(idx_ref, wr_hbm, tok_hbm, win_hbm, wout_hbm, y_hbm, meta_hbm, last_hbm,
            tok, key, send, recv, ret_p, ret_a0, ret_a1, ret_b0, ret_b1, win, wout, lhs, hid, meta, wr_ref, wr3,
            wr_sem, tok_sem, y_sem, meta_sem, win_sem, wout_sem,
            ds_sem, dr_sem, rs_sem, rr_sem):
    me = lax.axis_index("ep")

    def peer(k):
        return _peer(me, k)

    tok_copy = pltpu.make_async_copy(tok_hbm, tok, tok_sem)
    tok_copy.start()

    barrier = pltpu.get_barrier_semaphore()
    for k in range(1, NDEV):
        pl.semaphore_signal(barrier, inc=1, device_id={"ep": peer(k)}, device_id_type=MESH)

    def win_copy(e):
        return pltpu.make_async_copy(win_hbm.at[e], win.at[e % 2], win_sem.at[e % 2])

    def wout_copy(e):
        return pltpu.make_async_copy(wout_hbm.at[e], wout.at[e % 2], wout_sem.at[e % 2])

    before = (lax.broadcasted_iota(jnp.int32, (BLK, BLK), 0)
              < lax.broadcasted_iota(jnp.int32, (BLK, BLK), 1)).astype(F32).astype(BF16)
    expert_col = lax.broadcasted_iota(jnp.int32, (NEXP, BLK), 0)
    carry = jnp.zeros((NEXP, 1), F32)
    for b in range(NBLK):
        idx = idx_ref[:, b * BLK:(b + 1) * BLK]
        chosen = jnp.where(expert_col == idx, 1.0, 0.0).astype(F32)
        count = _dot(chosen.astype(BF16), before) + carry
        pos = jnp.sum(chosen * count, axis=0, keepdims=True)
        carry = carry + jnp.sum(chosen, axis=1, keepdims=True)
        slot = idx.astype(F32) * CAP + pos
        key[:, b * BLK:(b + 1) * BLK] = jnp.where(pos < CAP, slot, float(NEXP * CAP))

    tok_copy.wait()
    wr_copy = pltpu.make_async_copy(wr_hbm, wr_ref, wr_sem)
    wr_copy.start()
    for e in range(2):
        win_copy(e).start()
        wout_copy(e).start()

    def d_copy(k, h, j):
        rows = pl.ds(pl.multiple_of(h * HALF + D0[j], 16), DN[j])
        return pltpu.make_async_remote_copy(
            src_ref=send.at[k - 1, rows], dst_ref=recv.at[k, rows],
            send_sem=ds_sem.at[k - 1, h * 2 + j], recv_sem=dr_sem.at[k - 1, h * 2 + j],
            device_id={"ep": peer(k)}, device_id_type=MESH)

    def landing(k, h, j):
        if k == 1:
            return ret_p.at[pl.ds(pl.multiple_of(h * HALF + R0[j], 16), RN[j])]
        at = pl.ds((k - 2) * RN[j], RN[j])
        if h == 0:
            return (ret_a0, ret_a1)[j].at[at]
        if j == 0:
            return ret_b0.at[at]
        if k >= 6:
            return ret_b1.at[pl.ds((k - 6) * RN[1], RN[1])]
        return last_hbm.at[at]

    def r_copy(k, h, j):
        rows = pl.ds(pl.multiple_of(h * HALF + R0[j], 16), RN[j])
        return pltpu.make_async_remote_copy(
            src_ref=recv.at[k, rows], dst_ref=landing(k, h, j),
            send_sem=rs_sem.at[k - 1, h * 2 + j], recv_sem=rr_sem.at[k - 1, h * 2 + j],
            device_id={"ep": peer(k)}, device_id_type=MESH)

    order = (6, 7, 2, 4, 3, 5, 1)
    far = order[:-1]

    row_id = lax.broadcasted_iota(jnp.int32, (BLK, 1), 0)

    def dispatch(i, _):
        q = i // 4
        p = i % 4
        h = q // 2
        j = q % 2
        first = jnp.where(p == 0, 2, jnp.where(p == 1, 3, jnp.where(p == 2, 6, 0)))
        second = jnp.where(p == 0, 4, jnp.where(p == 1, 5, jnp.where(p == 2, 7, 1)))
        start = pl.multiple_of(h * HALF + j * 128, 16)
        base_a = peer(first) * ROWS + start
        base_b = peer(second) * ROWS + start - 128
        target = (row_id + jnp.where(row_id < 128, base_a, base_b)).astype(F32)
        hid[...] = jnp.where(key[...] == target, 1.0, 0.0).astype(BF16)
        rows = pl.ds(start, 128)
        for n in range(2):
            cols = slice(n * 512, (n + 1) * 512)
            part = _dot(hid[...], tok[:, cols]).astype(BF16)

            @pl.when(p < 3)
            def _():
                send[first - 1, rows, cols] = part[:128]

            @pl.when(p == 3)
            def _():
                recv[0, rows, cols] = part[:128]

            send[second - 1, rows, cols] = part[128:]
        @pl.when(i == 0)
        def _():
            pl.semaphore_wait(barrier, NDEV - 1)

        @pl.when(i < 4)
        def _():
            @pl.when(p < 3)
            def _():
                d_copy(first, 0, 0).start()
            d_copy(second, 0, 0).start()

        @pl.when(i == 9)
        def _():
            for k in order:
                d_copy(k, 0, 1).start()
        return 0

    lax.fori_loop(0, 16, dispatch, 0)

    eye = lax.broadcasted_iota(jnp.int32, (BLK, BLK), 0) == lax.broadcasted_iota(jnp.int32, (BLK, BLK), 1)
    lane = lax.broadcasted_iota(jnp.int32, (BLK, NEXP), 1).astype(F32)

    def router(b, _):
        at = pl.ds(pl.multiple_of(b * BLK, BLK), BLK)
        parts = _dot(tok[at, :], wr3[...])
        logits = parts[:, :NEXP] + parts[:, NEXP:2 * NEXP] + parts[:, 2 * NEXP:]
        top = jnp.max(logits, axis=1, keepdims=True)
        weight = jnp.exp(logits - top)
        total = jnp.sum(weight, axis=1, keepdims=True)
        idx_col = jnp.sum(jnp.where(eye, idx_ref[:, at].astype(F32), 0.0), axis=1, keepdims=True)
        slot_col = jnp.sum(jnp.where(eye, key[:, at], 0.0), axis=1, keepdims=True)
        gate = jnp.sum(jnp.where(lane == idx_col, weight / total, 0.0), axis=1, keepdims=True)
        meta[at, 0:1] = slot_col
        meta[at, 1:2] = gate
        return 0

    wr_copy.wait()
    top_bf16 = float(jnp.finfo(BF16).max)
    rest = wr_ref[...]
    for n in range(3):
        part = jnp.clip(rest, -top_bf16, top_bf16).astype(BF16)
        wr3[:, n * NEXP:(n + 1) * NEXP] = part
        rest = rest - part.astype(F32)

    lhs[...] = jnp.zeros_like(lhs)

    def group(g, _):
        h = g // 2
        j = g % 2

        @pl.when(g == 2)
        def _():
            lax.fori_loop(0, NBLK, router, 0)

        for jj in range(2):
            @pl.when(j == jj)
            def _():
                for k in order:
                    d_copy(k, h, jj).wait_recv()

                def spread(k, _):
                    at = pl.ds(pl.multiple_of(k * 32, 32), CAP)
                    block = recv.at[k, pl.ds(pl.multiple_of(h * HALF, 16), HALF)]
                    for c in range(4):
                        lo = (jj * 4 + c) * CAP
                        lhs[c, at, :] = block[lo:lo + CAP, :]
                    return 0

                lax.fori_loop(0, NDEV, spread, 0)

        def expert(c, _):
            e = g * 4 + c
            s = e % 2
            win_copy(e).wait()
            for lo, width in ((0, 768), (768, 768), (1536, 768), (2304, 512)):
                up = _dot(lhs[c], win[s, :, lo:lo + width])
                hid[:, lo:lo + width] = jnp.maximum(up, 0.0).astype(BF16)
            wout_copy(e).wait()
            for n in range(2):
                cols = slice(n * 512, (n + 1) * 512)
                lhs[c, :, cols] = _dot(hid[:, :HID], wout[s, :, cols]).astype(BF16)

            @pl.when(e + 2 < LOC)
            def _():
                win_copy(e + 2).start()
                wout_copy(e + 2).start()

            @pl.when(e == 1)
            def _():
                for k in order:
                    d_copy(k, 1, 0).start()

            @pl.when(e == 6)
            def _():
                for k in order:
                    d_copy(k, 1, 1).start()

            @pl.when(e == 9)
            def _():
                for k in far:
                    r_copy(k, 0, 0).start()

            @pl.when(e == 15)
            def _():
                for k in far:
                    r_copy(k, 0, 1).start()
            return 0

        lax.fori_loop(0, 4, expert, 0)

        for jj in range(2):
            @pl.when(j == jj)
            def _():
                def gather(k, _):
                    at = pl.ds(pl.multiple_of(k * 32, 32), CAP)
                    block = recv.at[k, pl.ds(pl.multiple_of(h * HALF, 16), HALF)]
                    for c in range(4):
                        lo = (jj * 4 + c) * CAP
                        block[lo:lo + CAP, :] = lhs[c, at, :]
                    return 0

                lax.fori_loop(0, NDEV, gather, 0)
                r_copy(1, h, jj).start()
        return 0

    lax.fori_loop(0, 4, group, 0)

    def y_copy(b):
        at = pl.ds(pl.multiple_of(b * BLK, BLK), BLK)
        return pltpu.make_async_copy(tok.at[at], y_hbm.at[at], y_sem.at[b])

    def combine(sources, first=False, last=False, midway=None, when=0):
        sources = [(_targets(me, pieces), rows) for pieces, rows in sources]

        def block(b, _):
            if last:
                @pl.when(b >= 1)
                def _():
                    y_copy(b - 1).start()
            if midway:
                pl.when(b == when)(midway)
            at = pl.ds(pl.multiple_of(b * BLK, BLK), BLK)
            total = _pick(meta[at, 0:1], sources)
            if not first:
                total = total + tok[at, :].astype(F32)
            tok[at, :] = total.astype(BF16)
            return 0

        lax.fori_loop(0, NBLK, block, 0, unroll=2)

    def arrived(peers, *chunks):
        for h, j in chunks:
            for k in peers:
                r_copy(k, h, j).wait_recv()

    meta_copy = pltpu.make_async_copy(meta, meta_hbm, meta_sem)
    meta_copy.start()
    arrived((1,), (0, 0), (0, 1), (1, 0), (1, 1))
    combine([([(0, 0, ROWS)], recv.at[0, :ROWS]), ([(1, 0, ROWS)], ret_p)], first=True)

    def start(peers, h, j):
        def go():
            for k in peers:
                r_copy(k, h, j).start()
        return go

    arrived(far, (0, 0))
    combine([([(k, R0[0], RN[0]) for k in range(2, 8)], ret_a0)], midway=start(far, 1, 0), when=4)
    arrived(far, (0, 1))
    combine([([(k, R0[1], RN[1]) for k in range(2, 8)], ret_a1)], midway=start((6, 7), 1, 1), when=8)
    arrived(far, (1, 0))
    start((2, 4, 3, 5), 1, 1)()
    combine([([(k, HALF, RN[0]) for k in range(2, 8)], ret_b0)])
    arrived((6, 7), (1, 1))
    combine([([(k, LAST, RN[1]) for k in (6, 7)], ret_b1)], last=True)
    y_copy(NBLK - 1).start()
    arrived((2, 3, 4, 5), (1, 1))

    for h in range(2):
        for j in range(2):
            for k in range(1, NDEV):
                d_copy(k, h, j).wait_send()
                r_copy(k, h, j).wait_send()
    for b in range(NBLK):
        y_copy(b).wait()
    meta_copy.wait()


def _finish(y_hbm, meta_hbm, last_hbm, out_hbm, y, meta, last, out, y_sem, meta_sem, last_sem, out_sem):
    me = lax.axis_index("ep")

    def rows(b):
        return pl.ds(pl.multiple_of(b * BLK, BLK), BLK)

    def y_copy(b):
        return pltpu.make_async_copy(y_hbm.at[rows(b)], y.at[rows(b)], y_sem.at[b])

    def out_copy(b):
        return pltpu.make_async_copy(out.at[rows(b)], out_hbm.at[rows(b)], out_sem.at[b])

    def meta_copy(b):
        return pltpu.make_async_copy(meta_hbm.at[rows(b)], meta.at[rows(b)], meta_sem.at[b])

    last_copy = pltpu.make_async_copy(last_hbm, last, last_sem)
    last_copy.start()
    for b in range(2):
        meta_copy(b).start()
        y_copy(b).start()
    target = _targets(me, [(k, LAST, RN[1]) for k in range(2, 6)])
    last_copy.wait()

    def block(b, _):
        @pl.when(b + 2 < NBLK)
        def _():
            meta_copy(b + 2).start()
            y_copy(b + 2).start()
        meta_copy(b).wait()
        y_copy(b).wait()
        total = _pick(meta[rows(b), 0:1], [(target, last)])
        total = total + y[rows(b), :].astype(F32)
        out[rows(b), :] = (meta[rows(b), 1:2] * total).astype(BF16)
        out_copy(b).start()
        return 0

    lax.fori_loop(0, NBLK, block, 0, unroll=2)
    for b in range(NBLK):
        out_copy(b).wait()


def solution(mesh):
    def local_block(tokens, expert_idx, w_router, w_in, w_out):
        any_space = pl.BlockSpec(memory_space=pl.ANY)
        vmem = pl.BlockSpec(memory_space=pltpu.VMEM)
        dma = pltpu.SemaphoreType.DMA
        partial, meta, last = pl.pallas_call(
            _kernel,
            out_shape=(jax.ShapeDtypeStruct((TOK, DIM), BF16),
                       jax.ShapeDtypeStruct((TOK, 128), F32),
                       jax.ShapeDtypeStruct((4 * RN[1], DIM), BF16)),
            in_specs=[vmem, any_space, any_space, any_space, any_space],
            out_specs=(any_space,) * 3,
            scratch_shapes=[
                pltpu.VMEM((TOK, DIM), BF16),
                pltpu.VMEM((1, TOK), F32),
                pltpu.VMEM((NDEV - 1, ROWS + 16, DIM), BF16),
                pltpu.VMEM((NDEV, ROWS + 16, DIM), BF16),
                pltpu.VMEM((ROWS, DIM), BF16),
                pltpu.VMEM((6 * RN[0], DIM), BF16),
                pltpu.VMEM((6 * RN[1], DIM), BF16),
                pltpu.VMEM((6 * RN[0], DIM), BF16),
                pltpu.VMEM((2 * RN[1], DIM), BF16),
                pltpu.VMEM((2, DIM, HID), BF16),
                pltpu.VMEM((2, HID, DIM), BF16),
                pltpu.VMEM((4, BLK, DIM), BF16),
                pltpu.VMEM((BLK, TOK), BF16),
                pltpu.VMEM((TOK, 128), F32),
                pltpu.VMEM((DIM, NEXP), F32),
                pltpu.VMEM((DIM, 3 * NEXP), BF16),
                dma, dma, dma((NBLK,)), dma, dma((2,)), dma((2,)),
                dma((NDEV - 1, 4)), dma((NDEV - 1, 4)), dma((NDEV - 1, 4)), dma((NDEV - 1, 4)),
            ],
            compiler_params=pltpu.CompilerParams(
                collective_id=0, has_side_effects=True, vmem_limit_bytes=67043328),
            name="moe_step",
        )(expert_idx.reshape(1, TOK), w_router, tokens, w_in, w_out)
        return pl.pallas_call(
            _finish,
            out_shape=jax.ShapeDtypeStruct((TOK, DIM), BF16),
            in_specs=[any_space] * 3,
            out_specs=any_space,
            scratch_shapes=[
                pltpu.VMEM((TOK, DIM), BF16),
                pltpu.VMEM((TOK, 128), F32),
                pltpu.VMEM((4 * RN[1], DIM), BF16),
                pltpu.VMEM((TOK, DIM), BF16),
                dma((NBLK,)), dma((NBLK,)), dma, dma((NBLK,)),
            ],
            compiler_params=pltpu.CompilerParams(vmem_limit_bytes=60 * 2**20),
            name="moe_finish",
        )(partial, meta, last)

    return jax.shard_map(
        local_block, mesh=mesh,
        in_specs=(P(("dp", "ep"), None), P(("dp", "ep")), P(None, None), P("ep", None, None), P("ep", None, None)),
        out_specs=P(("dp", "ep"), None), check_vma=False)
```
